32 devices in a mesh: chan: 4 (over y, x), slab: 8 (over z, core).
Axes of the slice: x: 2, y: 2, z: 4, core: 2. Of those that a mesh axis runs over, the one named last changes fastest.
Arguments:
- taylor_models: float32 [2, 2048, 2048], P(None, 'slab', 'chan'), may hold values from -6 to 6
- gridded_vis: bfloat16 [4, 2, 2048, 2048], P('chan', None, 'slab'), may hold values from -6 to 6
- uv_weight: bfloat16 [4, 2048, 2048], P('chan', 'slab'), may hold values from 0 to 2
- freq_ratio: float32 [4], P('chan'), may hold values from 0.6 to 1.4
- robust_scale: float32 [4], P('chan'), may hold values from 0.25 to 4
Outputs:
- taylor_residual: float32 [2, 2048, 2048], P(None, 'slab', 'chan')
The draws below stay inside these ranges and needn't reach their ends.
All inputs are finite; a program needn't handle non-finite values.
Results may differ from the reference program's by a relative error of at most 0.0003.
Values sent between devices are 32-bit elements; how exact they have to be, the bound alone decides.
A program may use at most 64 MiB of HBM per device.

```python
import math
import jax
import jax.numpy as jnp
from jax import lax

PIX = 2048
TERMS = 2
CHANNELS = 4


def levels(key, dims, cuts, smallest, largest):
    factor_of = 1.0
    for position, parts in cuts:
        steps = jax.random.uniform(jax.random.fold_in(jax.random.fold_in(key, 6), position), (parts,), jnp.float32, smallest / len(cuts), largest / len(cuts))
        factor_of = factor_of * jnp.repeat(jnp.exp(steps), dims[position] // parts).reshape((-1,) + (1,) * (len(dims) - 1 - position))
    return factor_of


def centred(own_key, extent, deviation, bound, pieces=(), dtype=jnp.bfloat16):
    entries = deviation * jax.random.normal(own_key, extent, jnp.float32)
    if pieces:
        entries = entries * levels(own_key, extent, pieces, -0.22, 0.18)
    return jnp.clip(entries, -bound, bound).astype(dtype)


def setup_inputs(seed: int = 0) -> dict:
    keys = jax.random.split(jax.random.key(seed), 6)
    taylor_models = centred(keys[0], (TERMS, PIX, PIX), 1.0, 6.0, ((1, 8), (2, 4)), jnp.float32)
    gridded_vis = centred(keys[1], (CHANNELS, 2, PIX, PIX), 1.0, 6.0, ((0, 4), (2, 8)))
    uv_weight = jnp.clip(2.0 * jax.random.uniform(keys[2], (CHANNELS, PIX, PIX), jnp.float32) ** levels(keys[2], (CHANNELS, PIX, PIX), ((0, 4), (1, 8)), -0.2, 0.2), 0.0, 2.0).astype(jnp.bfloat16)
    freq_ratio = jnp.clip(0.6 + 0.79999995 * jax.random.uniform(keys[3], (CHANNELS,), jnp.float32) ** levels(keys[3], (CHANNELS,), ((0, 4),), -0.2, 0.2), 0.6, 1.4)
    robust_scale = jnp.clip(jnp.exp(math.log(4.0) - 2.7725887 * jax.random.uniform(keys[4], (CHANNELS,), jnp.float32) ** levels(keys[4], (CHANNELS,), ((0, 4),), -0.2, 0.2)), 0.25, 4.0)
    return {"taylor_models": taylor_models, "gridded_vis": gridded_vis, "uv_weight": uv_weight, "freq_ratio": freq_ratio, "robust_scale": robust_scale}


def reference(taylor_models, gridded_vis, uv_weight, freq_ratio, robust_scale):
    def one_channel(carry, item):
        visible, weight, ratio, damping = item
        offset = ratio - 1.0
        sky_image = taylor_models[0]
        for term_index in range(1, TERMS):
            sky_image = sky_image + offset ** term_index * taylor_models[term_index]
        spectrum = jnp.fft.fft2(sky_image, norm="ortho").T
        visible_wide = visible.astype(jnp.float32)
        weight_wide = weight.astype(jnp.float32)
        delta_real = visible_wide[0] - weight_wide * jnp.real(spectrum)
        delta_imag = visible_wide[1] - weight_wide * jnp.imag(spectrum)
        robust = 1.0 / (1.0 + damping * (delta_real * delta_real + delta_imag * delta_imag))
        weighted = lax.complex(robust * delta_real, robust * delta_imag)
        residual = jnp.real(jnp.fft.ifft2(weighted.T, norm="ortho"))
        layers = [residual]
        for term_index in range(1, TERMS):
            layers.append(offset ** term_index * residual)
        return carry + jnp.stack(layers), None

    initial = jnp.zeros((TERMS, PIX, PIX), jnp.float32)
    total, _ = lax.scan(one_channel, initial, (gridded_vis, uv_weight, freq_ratio, robust_scale))
    return total
```

```python
import functools
import math

import jax
import jax.numpy as jnp
import numpy as np
from jax import lax
from jax.experimental import pallas as pl
from jax.experimental.pallas import tpu as pltpu
from jax.sharding import PartitionSpec as P

MESH = pl.DeviceIdType.MESH
TERMS = 2
RADIX = 16
LANES = 128
PARTS = 4


def fine_tables():
    points = RADIX * LANES
    j = np.arange(RADIX)[:, None, None]
    k = np.arange(LANES)[None, :, None]
    a = np.arange(LANES)[None, None, :]
    angle = 2.0 * np.pi / points * ((a * (RADIX * k + j)) % points)
    cos, sin = np.cos(angle), -np.sin(angle)
    full = np.concatenate(
        [np.concatenate([cos, -sin], axis=2), np.concatenate([sin, cos], axis=2)], axis=1
    ).astype(np.float32)
    back = np.ascontiguousarray(full.transpose(0, 2, 1))

    def halves(table):
        high = table.astype(jnp.bfloat16)
        low = (table - high.astype(np.float32)).astype(jnp.bfloat16)
        return np.stack([high, low])

    return halves(full), halves(back)


def swap_table(outer, inner):
    size = outer * inner
    table = np.zeros((size, size), np.float32)
    rows = np.arange(size)
    table[rows, (rows % inner) * outer + rows // inner] = 1.0
    return table.astype(jnp.bfloat16)


def plus(a, b):
    if a is None:
        return b
    return a if b is None else a + b


def minus(a, b):
    if b is None:
        return a
    return -b if a is None else a - b


def times(a, s):
    return None if a is None or s == 0.0 else a * s


def cadd(a, b):
    return plus(a[0], b[0]), plus(a[1], b[1])


def csub(a, b):
    return minus(a[0], b[0]), minus(a[1], b[1])


def turn(a, sign):
    if sign > 0:
        return minus(None, a[1]) if a[1] is not None else None, a[0]
    return a[1], minus(None, a[0]) if a[0] is not None else None


def ctwist(a, step, sign):
    step %= RADIX
    if step == 0:
        return a
    if step == 4:
        return turn(a, sign)
    c, s = math.cos(2 * math.pi * step / RADIX), sign * math.sin(2 * math.pi * step / RADIX)
    if step % 8 == 2:
        return times(minus(a[0], times(a[1], sign)), c), times(plus(times(a[0], sign), a[1]), c)
    return minus(times(a[0], c), times(a[1], s)), plus(times(a[0], s), times(a[1], c))


def four(a, b, c, d, sign):
    t0, t1, t2, t3 = cadd(a, c), csub(a, c), cadd(b, d), turn(csub(b, d), sign)
    return cadd(t0, t2), cadd(t1, t3), csub(t0, t2), csub(t1, t3)


def sixteen(x, sign):
    mid = [four(x[n], x[4 + n], x[8 + n], x[12 + n], sign) for n in range(4)]
    out = [None] * RADIX
    for k in range(4):
        tw = [ctwist(mid[n][k], n * k, sign) for n in range(4)]
        for q, y in enumerate(four(*tw, sign)):
            out[k + 4 * q] = y
    return out


def fine(table_ref, j, x):
    high = x.astype(jnp.bfloat16)
    low = (x - high.astype(jnp.float32)).astype(jnp.bfloat16)
    t_high, t_low = table_ref[0, j], table_ref[1, j]
    dot = functools.partial(jnp.dot, preferred_element_type=jnp.float32)
    return dot(t_high, high) + (dot(t_high, low) + dot(t_low, high))


def al8(i):
    return pl.multiple_of(i, 8)


def kernel(
    C, S,
    x_hbm, vis_hbm, wt_hbm, freq_ref, rob_ref, fwd_hbm, bwd_hbm, pu_hbm, pv_hbm,
    out_hbm,
    xr, xt, y_s, z_s, w_s, rs, rr, ms, mr, bs, br, ts, tr, x_s, zz_s, os_, fwd, bwd, pu, pv,
    raw, vt, offs,
    load_sem, x_send, x_recv, x_own, o_send, o_recv, o_own, f_send, f_recv,
    r_send, r_recv, r_own, m_send, m_recv, m_own, b_send, b_recv, b_own, t_send, t_recv, t_own,
):
    H = rs.shape[0]
    sub = x_hbm.shape[1] // C
    rows, cols = x_hbm.shape[1], x_hbm.shape[2]
    jper = RADIX // H
    kl = LANES // S
    piece = sub // PARTS
    scale = 1.0 / (RADIX * LANES)
    c_me, s_me = lax.axis_index("chan"), lax.axis_index("slab")
    chan_peers = [lax.rem(c_me + d, C) for d in range(1, C)]
    slab_peers = [lax.rem(s_me + d, S) for d in range(1, S)]

    def load(n):
        source, target = (
            (fwd_hbm, fwd),
            (vis_hbm.at[0], raw.at[pl.ds(0, 2)]),
            (wt_hbm, raw.at[pl.ds(2, 1)]),
            (pu_hbm, pu),
            (pv_hbm, pv),
            (bwd_hbm, bwd),
        )[n]
        return pltpu.make_async_copy(source, target, load_sem.at[n])

    def remote(src, dst, send, recv, **where):
        pltpu.make_async_remote_copy(
            src_ref=src, dst_ref=dst, send_sem=send, recv_sem=recv,
            device_id=where, device_id_type=MESH,
        ).start()

    def own(src, dst, sem):
        pltpu.make_async_copy(src, dst, sem).start()

    def landed(ref, sem):
        pltpu.make_async_copy(ref, ref, sem).wait()

    barrier = pltpu.get_barrier_semaphore()
    own(x_hbm.at[:, pl.ds(al8(sub * c_me), sub), :], xr.at[c_me], x_own)
    for n in range(6):
        load(n).start()
    for c in chan_peers:
        pl.semaphore_signal(barrier, inc=1, device_id={"chan": c}, device_id_type=MESH)
    for s in slab_peers:
        pl.semaphore_signal(barrier, inc=1, device_id={"slab": s}, device_id_type=MESH)
    pl.semaphore_wait(barrier, C + S - 2)

    for c in chan_peers:
        remote(
            x_hbm.at[:, pl.ds(al8(sub * c), sub), :], xr.at[c_me], x_send, x_recv, chan=c
        )
    own(freq_ref, offs.at[c_me], o_own)
    for c in chan_peers:
        remote(freq_ref, offs.at[c_me], f_send, f_recv, chan=c)

    def prep():
        for n in range(1, 5):
            load(n).wait()

        def body(n, carry):
            which, m = n // 8, n % 8
            block = raw[which, :, pl.ds(pl.multiple_of(m * 256, 256), 256)]
            turned = jnp.dot(pu[...], block, preferred_element_type=jnp.float32)
            flipped = lax.dot_general(
                pv[...], turned.astype(jnp.bfloat16), (((1,), (1,)), ((), ())),
                preferred_element_type=jnp.float32,
            ).astype(jnp.bfloat16)
            for h in range(H):
                for j in range(RADIX):
                    vt[which, h, j, pl.ds(pl.multiple_of(16 * m, 16), 16), :] = flipped[
                        16 * j : 16 * j + 16, LANES * h : LANES * (h + 1)
                    ]
            return carry

        lax.fori_loop(0, 24, body, 0)

    def rows_in():
        landed(xr.at[pl.ds(0, C - 1)], x_recv)
        landed(xr.at[0], x_own)
        load(0).wait()
        per = cols // LANES
        for b in range(RADIX):
            tile = xr[b // per, :, :, LANES * (b % per) : LANES * (b % per + 1)]
            xt[b] = tile.reshape(TERMS * sub, LANES).T

        def body(n, carry):
            at = al8(8 * n)
            out = sixteen([(xt[b, pl.ds(at, 8), :], None) for b in range(RADIX)], -1)
            for j in range(RADIX):
                for part in range(2):
                    value = out[j][part]
                    if value is None:
                        value = jnp.zeros((8, LANES), jnp.float32)
                    y_s[j, pl.ds(al8(part * LANES + at), 8), :] = value
            return carry

        lax.fori_loop(0, LANES // 8, body, 0)

    def rows_out(h):
        def body(jl, carry):
            z = fine(fwd, jper * h + jl, y_s[jper * h + jl])
            for s in range(S):
                for part in range(2):
                    w_s[s, part, pl.ds(al8(kl * jl), kl), :] = z[
                        part * LANES + kl * s : part * LANES + kl * (s + 1), :
                    ]
            return carry

        lax.fori_loop(0, jper, body, 0)

        def flip(s, carry):
            for part in range(2):
                rs[h, s, part] = w_s[s, part].T.reshape(TERMS, sub, LANES)
            return carry

        lax.fori_loop(0, S, flip, 0)
        for q in range(PARTS):
            span = pl.ds(q * piece, piece)
            own(rs.at[h, s_me, :, :, span, :], rr.at[h, s_me, :, :, span, :], r_own.at[h, q])
            for s in slab_peers:
                remote(
                    rs.at[h, s, :, :, span, :], rr.at[h, s_me, :, :, span, :],
                    r_send, r_recv.at[h, q], slab=s,
                )

    def mix(h, q):
        span = pl.ds(q * piece, piece)
        landed(rr.at[h, pl.ds(0, S - 1), :, :, span, :], r_recv.at[h, q])
        landed(rr.at[h, 0, :, :, span, :], r_own.at[h, q])

        def body(s, carry):
            base = rr[h, s, :, 0, span, :] * scale
            slope = rr[h, s, :, 1, span, :] * scale
            for c in range(C):
                offset = offs[c, 0:1, :] - 1.0
                ms[h, c, :, s, span, :] = base + offset[None] * slope
            return carry

        lax.fori_loop(0, S, body, 0)
        there = pl.ds(al8(sub * c_me + q * piece), piece)
        own(ms.at[h, c_me, :, :, span, :], mr.at[h, :, :, there, :], m_own.at[h])
        for c in chan_peers:
            remote(
                ms.at[h, c, :, :, span, :], mr.at[h, :, :, there, :],
                m_send, m_recv.at[h], chan=c,
            )

    def column_in(h):
        landed(ms.at[h, pl.ds(0, C - 1)], m_recv.at[h])
        landed(ms.at[h, 0], m_own.at[h])

        def body(n, carry):
            at = 8 * n
            x = []
            for b in range(RADIX):
                s, row = LANES * b // rows, LANES * b % rows
                x.append(tuple(mr[h, part, s, pl.ds(al8(row + at), 8), :] for part in range(2)))
            out = sixteen(x, -1)
            for j in range(RADIX):
                for part in range(2):
                    y_s[j, pl.ds(al8(part * LANES + at), 8), :] = out[j][part]
            return carry

        lax.fori_loop(0, LANES // 8, body, 0)

    def column_mid(h):
        def body(j, carry):
            z = fine(fwd, j, y_s[j])
            weight = vt[2, h, j].astype(jnp.float32)
            real = vt[0, h, j].astype(jnp.float32) - weight * z[:LANES]
            imag = vt[1, h, j].astype(jnp.float32) - weight * z[LANES:]
            robust = 1.0 / (1.0 + rob_ref[0] * (real * real + imag * imag))
            z_s[j] = fine(bwd, j, jnp.concatenate([robust * real, robust * imag], axis=0))
            return carry

        lax.fori_loop(0, RADIX, body, 0)

    def column_out(h, q):
        per = piece // 8

        def body(n, carry):
            at = sub * (n // per) + q * piece + 8 * (n % per)
            out = sixteen(
                [tuple(z_s[j, pl.ds(al8(part * LANES + at), 8), :] for part in range(2)) for j in range(RADIX)],
                1,
            )
            for b in range(RADIX):
                s, row = LANES * b // rows, LANES * b % rows
                for part in range(2):
                    bs[h, part, s, pl.ds(al8(row + at), 8), :] = out[b][part]
            return carry

        lax.fori_loop(0, LANES // sub * per, body, 0)
        span = pl.ds(q * piece, piece)
        here = lambda c: pl.ds(al8(sub * c + q * piece), piece)
        own(bs.at[h, :, :, here(c_me), :], br.at[h, c_me, :, :, span, :], b_own.at[h, q])
        for c in chan_peers:
            remote(
                bs.at[h, :, :, here(c), :], br.at[h, c_me, :, :, span, :],
                b_send, b_recv.at[h, q], chan=c,
            )

    def gather(h, q):
        span = pl.ds(q * piece, piece)
        landed(br.at[h, pl.ds(0, C - 1), :, :, span, :], b_recv.at[h, q])
        landed(br.at[h, 0, :, :, span, :], b_own.at[h, q])

        def body(s, carry):
            base, slope = None, None
            for c in range(C):
                offset = (offs[c, 0:1, :] - 1.0)[None]
                value = br[h, c, :, s, span, :]
                base = value if base is None else base + value
                slope = offset * value if slope is None else slope + offset * value
            ts[h, s, :, 0, span, :] = base * scale
            ts[h, s, :, 1, span, :] = slope * scale
            return carry

        lax.fori_loop(0, S, body, 0)
        own(ts.at[h, s_me, :, :, span, :], tr.at[h, s_me, :, :, span, :], t_own.at[h])
        for s in slab_peers:
            remote(
                ts.at[h, s, :, :, span, :], tr.at[h, s_me, :, :, span, :],
                t_send, t_recv.at[h], slab=s,
            )

    def back_in(h):
        landed(tr.at[h, pl.ds(0, S - 1)], t_recv.at[h])
        landed(tr.at[h, 0], t_own.at[h])

        def flip(s, carry):
            for part in range(2):
                tile = tr[h, s, part].reshape(TERMS * sub, LANES).T
                for jl in range(jper):
                    x_s[jper * h + jl, pl.ds(al8(part * LANES + kl * s), kl), :] = tile[
                        kl * jl : kl * (jl + 1), :
                    ]
            return carry

        lax.fori_loop(0, S, flip, 0)

        def body(jl, carry):
            zz_s[jper * h + jl] = fine(bwd, jper * h + jl, x_s[jper * h + jl])
            return carry

        lax.fori_loop(0, jper, body, 0)

    def back_out():
        def body(n, carry):
            at = 8 * n
            out = sixteen(
                [tuple(zz_s[j, pl.ds(al8(part * LANES + at), 8), :] for part in range(2)) for j in range(RADIX)],
                1,
            )
            for b in range(RADIX):
                xt[b, pl.ds(al8(at), 8), :] = out[b][0]
            return carry

        lax.fori_loop(0, LANES // 8, body, 0)
        per = cols // LANES
        for b in range(RADIX):
            os_[b // per, :, :, LANES * (b % per) : LANES * (b % per + 1)] = xt[b].T.reshape(
                TERMS, sub, LANES
            )
        there = pl.ds(al8(sub * c_me), sub)
        for c in chan_peers:
            remote(os_.at[c], out_hbm.at[:, there, :], o_send, o_recv, chan=c)
        own(os_.at[c_me], out_hbm.at[:, there, :], o_own)

    prep()
    landed(offs.at[pl.ds(0, C - 1)], f_recv)
    landed(offs.at[0], o_own)
    rows_in()
    for h in range(H):
        rows_out(h)
    for h in range(H):
        for q in range(PARTS):
            mix(h, q)
    load(5).wait()
    for h in range(H):
        column_in(h)
        column_mid(h)
        for q in range(PARTS):
            column_out(h, q)
    for h in range(H):
        for q in range(PARTS):
            gather(h, q)
    for h in range(H):
        back_in(h)
    back_out()

    landed(xr.at[pl.ds(0, C - 1)], x_send)
    landed(offs.at[pl.ds(0, C - 1)], f_send)
    landed(rs.at[:, pl.ds(0, S - 1)], r_send)
    landed(ms.at[:, pl.ds(0, C - 1)], m_send)
    landed(br.at[:, pl.ds(0, C - 1)], b_send)
    landed(ts.at[:, pl.ds(0, S - 1)], t_send)
    landed(os_.at[pl.ds(0, C - 1)], o_send)
    landed(os_.at[pl.ds(0, C - 1)], o_recv)
    landed(os_.at[0], o_own)


def tiled(taylor_models, gridded_vis, uv_weight, freq_ratio, robust_scale):
    C, S = lax.axis_size("chan"), lax.axis_size("slab")
    terms, rows, cols = taylor_models.shape
    sub = rows // C
    U = gridded_vis.shape[2]
    H = U // LANES
    fwd, bwd = fine_tables()
    pu, pv = swap_table(RADIX, U // RADIX), swap_table(RADIX, 16)
    freq = jnp.broadcast_to(freq_ratio[:, None], (8, LANES))
    f32, bf16 = jnp.float32, jnp.bfloat16
    stage = (RADIX, 2 * LANES, LANES)
    slabbed = (H, S, 2, terms, sub, LANES)
    chanbed = (H, C, 2, S, sub, LANES)
    natural = (H, 2, S, rows, LANES)
    V = lambda shape, dtype=f32: pltpu.VMEM(shape, dtype)
    D = pltpu.SemaphoreType.DMA
    anywhere = pl.BlockSpec(memory_space=pl.ANY)
    return pl.pallas_call(
        functools.partial(kernel, C, S),
        out_shape=jax.ShapeDtypeStruct(taylor_models.shape, f32),
        in_specs=[
            anywhere, anywhere, anywhere,
            pl.BlockSpec(memory_space=pltpu.VMEM), pl.BlockSpec(memory_space=pltpu.SMEM),
            anywhere, anywhere, anywhere, anywhere,
        ],
        out_specs=anywhere,
        scratch_shapes=[
            V((C, terms, sub, cols)), V((RADIX, LANES, LANES)), V(stage), V(stage),
            V((S, 2, LANES, LANES)), V(slabbed), V(slabbed), V(chanbed), V(natural),
            V(natural), V(chanbed), V(slabbed), V(slabbed), V(stage), V(stage),
            V((C, terms, sub, cols)), V(fwd.shape, bf16), V(bwd.shape, bf16),
            V(pu.shape, bf16), V(pv.shape, bf16),
            V((3, U, RADIX * LANES), bf16), V((3, H, RADIX, LANES, LANES), bf16),
            V((C, 8, LANES)),
            D((6,)), D(()), D(()), D(()), D(()), D(()), D(()), D(()), D(()),
            D(()), D((H, PARTS)), D((H, PARTS)),
            D(()), D((H,)), D((H,)),
            D(()), D((H, PARTS)), D((H, PARTS)),
            D(()), D((H,)), D((H,)),
        ],
        compiler_params=pltpu.CompilerParams(
            collective_id=0, has_side_effects=True, vmem_limit_bytes=63 * 1024 * 1024
        ),
    )(taylor_models, gridded_vis, uv_weight, freq, robust_scale, fwd, bwd, pu, pv)


HIGHEST = lax.Precision.HIGH


def dft_table(points, direction):
    steps_all = jnp.arange(points, dtype=jnp.int32)
    product = steps_all[:, None] * steps_all[None, :] % points
    angles = product.astype(jnp.float32) * (2.0 * math.pi / points)
    return (jnp.cos(angles), direction * jnp.sin(angles))


def twiddle_table(outer_points, inner_points, direction):
    outer_steps = jnp.arange(outer_points, dtype=jnp.int32)
    inner_steps = jnp.arange(inner_points, dtype=jnp.int32)
    overall = outer_points * inner_points
    product = outer_steps[:, None] * inner_steps[None, :] % overall
    angles = product.astype(jnp.float32) * (2.0 * math.pi / overall)
    return (jnp.cos(angles), direction * jnp.sin(angles))


def complex_product(formula, left_real, left_imag, table_real, table_imag):
    out_real = jnp.einsum(formula, left_real, table_real, precision=HIGHEST) - jnp.einsum(
        formula, left_imag, table_imag, precision=HIGHEST
    )
    out_imag = jnp.einsum(formula, left_real, table_imag, precision=HIGHEST) + jnp.einsum(
        formula, left_imag, table_real, precision=HIGHEST
    )
    return (out_real, out_imag)


def rotate(left_real, left_imag, table_real, table_imag):
    return (
        left_real * table_real - left_imag * table_imag,
        left_real * table_imag + left_imag * table_real,
    )


def general(taylor_models, gridded_vis, uv_weight, freq_ratio, robust_scale):
    inner_count = 128
    PIX = taylor_models.shape[2] * lax.axis_size("chan")
    outer_count = PIX // inner_count
    chans = lax.axis_size("chan")
    slabs = lax.axis_size("slab")
    rows = taylor_models.shape[1]
    cols = taylor_models.shape[2]
    sub = rows // chans
    col_count = PIX // slabs
    outer_cos, outer_sin = dft_table(outer_count, -1.0)
    inner_cos, inner_sin = dft_table(inner_count, -1.0)
    twist_cos, twist_sin = twiddle_table(outer_count, inner_count, -1.0)
    offsets = lax.all_gather(freq_ratio, "chan", axis=0, tiled=True) - 1.0

    pieces = taylor_models.reshape(TERMS, chans, sub, cols).transpose(1, 0, 2, 3)
    pieces = lax.all_to_all(pieces, "chan", split_axis=0, concat_axis=0, tiled=True)
    layered = pieces.transpose(1, 2, 0, 3).reshape(TERMS * sub, outer_count, inner_count)
    part_real = jnp.einsum("yba,jb->yja", layered, outer_cos, precision=HIGHEST)
    part_imag = jnp.einsum("yba,jb->yja", layered, outer_sin, precision=HIGHEST)
    turned_real, turned_imag = rotate(part_real, part_imag, twist_cos, twist_sin)
    spec_real, spec_imag = complex_product(
        "yja,ka->kjy", turned_real, turned_imag, inner_cos, inner_sin
    )
    outgoing = jnp.stack(
        [
            spec_real.reshape(slabs, col_count, TERMS * sub),
            spec_imag.reshape(slabs, col_count, TERMS * sub),
        ],
        axis=1,
    )
    arrived = lax.all_to_all(outgoing, "slab", split_axis=0, concat_axis=0, tiled=True)
    arrived = arrived.reshape(slabs, 2, col_count, TERMS, sub)
    arrived = arrived.transpose(3, 1, 2, 0, 4).reshape(TERMS, 2, col_count, slabs * sub)
    mixed = arrived[0][None] + offsets[:, None, None, None] * arrived[1][None]
    mixed = lax.all_to_all(mixed, "chan", split_axis=0, concat_axis=0, tiled=True)
    columns = mixed.reshape(chans, 2, col_count, slabs, sub).transpose(1, 2, 3, 0, 4)
    layered_cols = columns.reshape(2, col_count, outer_count, inner_count)
    part_real, part_imag = complex_product(
        "uba,jb->uja", layered_cols[0], layered_cols[1], outer_cos, outer_sin
    )
    turned_real, turned_imag = rotate(part_real, part_imag, twist_cos, twist_sin)
    freq_real, freq_imag = complex_product(
        "uja,ka->ujk", turned_real, turned_imag, inner_cos, inner_sin
    )
    freq_real = freq_real / PIX
    freq_imag = freq_imag / PIX
    weight = (
        uv_weight[0]
        .astype(jnp.float32)
        .reshape(col_count, inner_count, outer_count)
        .transpose(0, 2, 1)
    )
    visible = (
        gridded_vis[0]
        .astype(jnp.float32)
        .reshape(2, col_count, inner_count, outer_count)
        .transpose(0, 1, 3, 2)
    )
    delta_real = visible[0] - weight * freq_real
    delta_imag = visible[1] - weight * freq_imag
    robust = 1.0 / (1.0 + robust_scale[0] * (delta_real * delta_real + delta_imag * delta_imag))
    weighted_real = robust * delta_real
    weighted_imag = robust * delta_imag
    back_real, back_imag = complex_product(
        "ujk,ak->uja", weighted_real, weighted_imag, inner_cos, -inner_sin
    )
    back_real, back_imag = rotate(back_real, back_imag, twist_cos, -twist_sin)
    back_real, back_imag = complex_product(
        "uja,bj->uba", back_real, back_imag, outer_cos, -outer_sin
    )
    back = jnp.stack([back_real, back_imag]).reshape(2, col_count, slabs, chans, sub)
    back = back.transpose(3, 0, 1, 2, 4).reshape(chans, 2, col_count, slabs * sub)
    back = lax.all_to_all(back, "chan", split_axis=0, concat_axis=0, tiled=True)
    total = jnp.stack(
        [jnp.sum(back * offsets[:, None, None, None] ** t, axis=0) for t in range(TERMS)]
    )
    total = total.reshape(TERMS, 2, col_count, slabs, sub).transpose(3, 1, 2, 0, 4)
    total = total.reshape(slabs, 2, col_count, TERMS * sub)
    total = lax.all_to_all(total, "slab", split_axis=0, concat_axis=0, tiled=True)
    layered_rows = total.transpose(1, 0, 2, 3).reshape(2, inner_count, outer_count, TERMS * sub)
    last_real, last_imag = complex_product(
        "kjy,ak->ajy", layered_rows[0], layered_rows[1], inner_cos, -inner_sin
    )
    last_real, last_imag = rotate(
        last_real, last_imag, twist_cos.T[:, :, None], -twist_sin.T[:, :, None]
    )
    image_out = jnp.einsum("ajy,bj->yba", last_real, outer_cos, precision=HIGHEST) + jnp.einsum(
        "ajy,bj->yba", last_imag, outer_sin, precision=HIGHEST
    )
    image_out = image_out.reshape(TERMS, sub, chans, cols).transpose(2, 0, 1, 3) / PIX
    tiles = lax.all_to_all(image_out, "chan", split_axis=0, concat_axis=0, tiled=True)
    return tiles.transpose(1, 0, 2, 3).reshape(TERMS, rows, cols)


def local(taylor_models, gridded_vis, uv_weight, freq_ratio, robust_scale):
    C, S = lax.axis_size("chan"), lax.axis_size("slab")
    terms, rows, cols = taylor_models.shape
    pix, sub, U = cols * C, rows // C, gridded_vis.shape[2]
    fits = (
        terms == TERMS
        and pix == RADIX * LANES
        and rows * S == pix
        and rows % LANES == 0
        and cols % LANES == 0
        and terms * sub == LANES
        and sub % (8 * PARTS) == 0
        and LANES % (8 * S) == 0
        and U % LANES == 0
    )
    form = tiled if fits else general
    return form(taylor_models, gridded_vis, uv_weight, freq_ratio, robust_scale)


def solution(mesh):
    placed = (
        P(None, "slab", "chan"),
        P("chan", None, "slab", None),
        P("chan", "slab", None),
        P("chan"),
        P("chan"),
    )
    return jax.shard_map(
        local, mesh=mesh, in_specs=placed, out_specs=P(None, "slab", "chan"), check_vma=False
    )
```

```python
import functools
import math

import jax
import jax.numpy as jnp
import numpy as np
from jax import lax
from jax.experimental import pallas as pl
from jax.experimental.pallas import tpu as pltpu
from jax.sharding import PartitionSpec as P

MESH = pl.DeviceIdType.MESH
TERMS = 2
RADIX = 16
LANES = 128
PARTS = 4
NEAR, FAR = 0, 1
BACK_DEPTH = 2
HALVES = 4


def fine_tables():
    points = RADIX * LANES
    j = np.arange(RADIX)[:, None, None]
    k = np.arange(LANES)[None, :, None]
    a = np.arange(LANES)[None, None, :]
    angle = 2.0 * np.pi / points * ((a * (RADIX * k + j)) % points)
    cos, sin = np.cos(angle), -np.sin(angle)

    def halves(real, imag):
        table = np.concatenate([real, imag], axis=1).astype(np.float32)
        high = table.astype(jnp.bfloat16)
        low = (table - high.astype(np.float32)).astype(jnp.bfloat16)
        return np.concatenate([high, low], axis=2)

    flip = lambda t: t.transpose(0, 2, 1)
    return halves(cos, sin), halves(flip(cos), -flip(sin))


def swap_table(outer, inner):
    size = outer * inner
    table = np.zeros((size, size), np.float32)
    rows = np.arange(size)
    table[rows, (rows % inner) * outer + rows // inner] = 1.0
    return table.astype(jnp.bfloat16)


def plus(a, b):
    if a is None:
        return b
    return a if b is None else a + b


def minus(a, b):
    if b is None:
        return a
    return -b if a is None else a - b


def times(a, s):
    return None if a is None or s == 0.0 else a * s


def cadd(a, b):
    return plus(a[0], b[0]), plus(a[1], b[1])


def csub(a, b):
    return minus(a[0], b[0]), minus(a[1], b[1])


def turn(a, sign):
    if sign > 0:
        return minus(None, a[1]) if a[1] is not None else None, a[0]
    return a[1], minus(None, a[0]) if a[0] is not None else None


def ctwist(a, step, sign):
    step %= RADIX
    if step == 0:
        return a
    if step == 4:
        return turn(a, sign)
    c, s = math.cos(2 * math.pi * step / RADIX), sign * math.sin(2 * math.pi * step / RADIX)
    if step % 8 == 2:
        return times(minus(a[0], times(a[1], sign)), c), times(plus(times(a[0], sign), a[1]), c)
    return minus(times(a[0], c), times(a[1], s)), plus(times(a[0], s), times(a[1], c))


def four(a, b, c, d, sign):
    t0, t1, t2, t3 = cadd(a, c), csub(a, c), cadd(b, d), turn(csub(b, d), sign)
    return cadd(t0, t2), cadd(t1, t3), csub(t0, t2), csub(t1, t3)


def sixteen(x, sign):
    mid = [four(x[n], x[4 + n], x[8 + n], x[12 + n], sign) for n in range(4)]
    out = [None] * RADIX
    for k in range(4):
        tw = [ctwist(mid[n][k], n * k, sign) for n in range(4)]
        for q, y in enumerate(four(*tw, sign)):
            out[k + 4 * q] = y
    return out


def fine(table, x):
    high = x.astype(jnp.bfloat16)
    low = (x - high.astype(jnp.float32)).astype(jnp.bfloat16)
    t_high, t_low = table[:, :LANES], table[:, LANES:]
    left = jnp.concatenate(
        [jnp.concatenate([t_high, t_high], axis=1), jnp.concatenate([t_low, t_low], axis=1)], axis=0
    )
    out = jnp.dot(left, jnp.concatenate([high, low], axis=0), preferred_element_type=jnp.float32)
    out = out[: 2 * LANES] + out[2 * LANES :]
    real = out[:LANES, :LANES] - out[LANES:, LANES:]
    imag = out[:LANES, LANES:] + out[LANES:, :LANES]
    return real, imag


def put(ref, *index, at, value):
    for part in range(2):
        v = value[part]
        if v is None:
            v = jnp.zeros((8, LANES), jnp.float32)
        ref[(*index, pl.ds(al8(at), 8), pl.ds(part * LANES, LANES))] = v


def get(ref, *index, at):
    return tuple(ref[(*index, pl.ds(al8(at), 8), pl.ds(part * LANES, LANES))] for part in range(2))


def al8(i):
    return pl.multiple_of(i, 8)


def kernel(
    C, S,
    x_hbm, vis_hbm, wt_hbm, freq_ref, rob_ref, fwd_hbm, bwd_hbm, pu_hbm, pv_hbm,
    out_hbm,
    xr, xt, y_s, z_s, w_s, rs, rr, ms, mr, bs, br, ts, tr, x_s, os_, fwd, bwd, pu, pv,
    raw, vt, offs,
    load_sem, x_send, x_recv, x_own, o_send, o_recv, o_own, o_done, f_send, f_recv,
    r_send, r_recv, r_own, m_send, m_recv, m_own, b_send, b_recv, b_own, t_send, t_recv, t_own,
):
    H = rs.shape[0]
    sub = x_hbm.shape[1] // C
    rows, cols = x_hbm.shape[1], x_hbm.shape[2]
    jper = RADIX // H
    kl = LANES // S
    piece = sub // PARTS
    scale = 1.0 / (RADIX * LANES)
    c_me, s_me = lax.axis_index("chan"), lax.axis_index("slab")
    chan_peers = [lax.rem(c_me + d, C) for d in range(1, C)]
    if C == 4:
        chan_peers = [3 - c_me, c_me + 1 - 2 * lax.rem(c_me, 2), lax.rem(c_me + 2, 4)]
    G = S // 2
    low = s_me // G * G
    first_of = (low, G - low)
    slab_peers = (
        [low + lax.rem(s_me + d, G) for d in range(1, G)],
        [G - low + lax.rem(s_me + d, G) for d in range(G)],
    )

    def load(n):
        source, target = (
            (fwd_hbm, fwd),
            (vis_hbm.at[0], raw.at[pl.ds(0, 2)]),
            (wt_hbm, raw.at[pl.ds(2, 1)]),
            (pu_hbm, pu),
            (pv_hbm, pv),
            (bwd_hbm, bwd),
        )[n]
        return pltpu.make_async_copy(source, target, load_sem.at[n])

    def remote(src, dst, send, recv, **where):
        pltpu.make_async_remote_copy(
            src_ref=src, dst_ref=dst, send_sem=send, recv_sem=recv,
            device_id=where, device_id_type=MESH,
        ).start()

    def own(src, dst, sem):
        pltpu.make_async_copy(src, dst, sem).start()

    def landed(ref, sem):
        pltpu.make_async_copy(ref, ref, sem).wait()

    half = sub // HALVES
    halved = lambda p: pl.ds(p * half, half)
    wide = TERMS * half

    barrier = pltpu.get_barrier_semaphore()
    for c in chan_peers:
        pl.semaphore_signal(barrier, inc=1, device_id={"chan": c}, device_id_type=MESH)
    for s in slab_peers[NEAR] + slab_peers[FAR]:
        pl.semaphore_signal(barrier, inc=1, device_id={"slab": s}, device_id_type=MESH)
    for p in range(HALVES):
        own(
            x_hbm.at[:, pl.ds(al8(sub * c_me + p * half), half), :],
            xr.at[c_me, :, halved(p), :], x_own.at[p],
        )
    own(freq_ref, offs.at[c_me], o_own)
    for n in range(6):
        load(n).start()
    pl.semaphore_wait(barrier, C + S - 2)

    for p in range(HALVES):
        for c in chan_peers:
            remote(
                x_hbm.at[:, pl.ds(al8(sub * c + p * half), half), :],
                xr.at[c_me, :, halved(p), :], x_send, x_recv.at[p], chan=c,
            )
    for c in chan_peers:
        remote(freq_ref, offs.at[c_me], f_send, f_recv, chan=c)

    def prep(which, first, last):
        def body(m, carry):
            block = raw[which, :, pl.ds(pl.multiple_of(m * 256, 256), 256)]
            turned = jnp.dot(pu[...], block, preferred_element_type=jnp.float32)
            flipped = lax.dot_general(
                pv[...], turned.astype(jnp.bfloat16), (((1,), (1,)), ((), ())),
                preferred_element_type=jnp.float32,
            ).astype(jnp.bfloat16)
            for h in range(H):
                for j in range(RADIX):
                    vt[which, h, j, pl.ds(pl.multiple_of(16 * m, 16), 16), :] = flipped[
                        16 * j : 16 * j + 16, LANES * h : LANES * (h + 1)
                    ]
            return carry

        lax.fori_loop(first, last, body, 0)

    def rows_in(p):
        landed(xr.at[pl.ds(0, C - 1), :, halved(p), :], x_recv.at[p])
        landed(xr.at[0, :, halved(p), :], x_own.at[p])
        per = cols // LANES
        for b in range(RADIX):
            tile = xr[b // per, :, halved(p), LANES * (b % per) : LANES * (b % per + 1)]
            xt[b, :, 0:wide] = tile.reshape(wide, LANES).T

        def body(n, carry):
            out = sixteen([(xt[b, pl.ds(al8(8 * n), 8), :], None) for b in range(RADIX)], -1)
            for j in range(RADIX):
                put(y_s, p, j, at=8 * n, value=out[j])
            return carry

        lax.fori_loop(0, LANES // 8, body, 0)

    def rows_out(h, p):
        def body(jl, carry):
            z = fine(fwd[jper * h + jl], y_s[p, jper * h + jl])
            for s in range(S):
                for part in range(2):
                    w_s[s, part, pl.ds(al8(kl * jl), kl), :] = z[part][kl * s : kl * (s + 1), :]
            return carry

        lax.fori_loop(0, jper, body, 0, unroll=2)

        def flip(s, carry):
            for part in range(2):
                rs[h, s, part, :, halved(p), :] = w_s[s, part, :, 0:wide].T.reshape(TERMS, half, LANES)
            return carry

        lax.fori_loop(0, S, flip, 0)

    def to_slabs(source, target, g, n, send, recv, done):
        h, q = n // PARTS, n % PARTS
        span = pl.ds(q * piece, piece)
        for s in slab_peers[g]:
            remote(
                source.at[h, s, :, :, span, :], target.at[h, s_me, :, :, span, :],
                send, recv.at[g, h, q], slab=s,
            )
        if g == NEAR:
            own(
                source.at[h, s_me, :, :, span, :], target.at[h, s_me, :, :, span, :],
                done.at[h, q],
            )

    def from_slabs(target, g, n, recv, done):
        h, q = n // PARTS, n % PARTS
        span = pl.ds(q * piece, piece)
        landed(target.at[h, pl.ds(0, len(slab_peers[g])), :, :, span, :], recv.at[g, h, q])
        if g == NEAR:
            landed(target.at[h, 0, :, :, span, :], done.at[h, q])

    def send_rows(g, n):
        to_slabs(rs, rr, g, n, r_send, r_recv, r_own)

    def mix(g, n):
        h, q = n // PARTS, n % PARTS
        span = pl.ds(q * piece, piece)
        from_slabs(rr, g, n, r_recv, r_own)

        def body(i, carry):
            s = first_of[g] + i
            base = rr[h, s, :, 0, span, :] * scale
            slope = rr[h, s, :, 1, span, :] * scale
            for c in range(C):
                offset = offs[c, 0:1, :] - 1.0
                ms[h, c, :, s, span, :] = base + offset[None] * slope
            return carry

        lax.fori_loop(0, G, body, 0)
        there = pl.ds(al8(sub * c_me + q * piece), piece)
        group = pl.ds(first_of[g], G)
        for c in chan_peers:
            remote(
                ms.at[h, c, :, group, span, :], mr.at[h, :, group, there, :],
                m_send, m_recv.at[h], chan=c,
            )
        own(ms.at[h, c_me, :, group, span, :], mr.at[h, :, group, there, :], m_own.at[h])

    def column_in(h):
        landed(ms.at[h, pl.ds(0, C - 1)], m_recv.at[h])
        landed(ms.at[h, 0], m_own.at[h])

        def body(n, carry):
            at = 8 * n
            x = []
            for b in range(RADIX):
                s, row = LANES * b // rows, LANES * b % rows
                x.append(tuple(mr[h, part, s, pl.ds(al8(row + at), 8), :] for part in range(2)))
            out = sixteen(x, -1)
            for j in range(RADIX):
                put(y_s, h, j, at=at, value=out[j])
            return carry

        lax.fori_loop(0, LANES // 8, body, 0)

    def column_mid(h, first, last):
        def body(j, carry):
            zr, zi = fine(fwd[j], y_s[h, j])
            weight = vt[2, h, j].astype(jnp.float32)
            real = vt[0, h, j].astype(jnp.float32) - weight * zr
            imag = vt[1, h, j].astype(jnp.float32) - weight * zi
            robust = 1.0 / (1.0 + rob_ref[0] * (real * real + imag * imag))
            zr, zi = fine(bwd[j], jnp.concatenate([robust * real, robust * imag], axis=1))
            z_s[h, j, :, 0:LANES] = zr
            z_s[h, j, :, LANES : 2 * LANES] = zi
            return carry

        lax.fori_loop(first, last, body, 0, unroll=2)

    def column_out(h):
        def body(n, carry):
            out = sixteen([get(z_s, h, j, at=8 * n) for j in range(RADIX)], 1)
            for b in range(RADIX):
                s, row = LANES * b // rows, LANES * b % rows
                for part in range(2):
                    bs[h, part, s, pl.ds(al8(row + 8 * n), 8), :] = out[b][part]
            return carry

        lax.fori_loop(0, LANES // 8, body, 0)

    def send_back(g, n):
        h, q = n // PARTS, n % PARTS
        span = pl.ds(q * piece, piece)
        group = pl.ds(first_of[g], G)
        here = lambda c: pl.ds(al8(sub * c + q * piece), piece)
        for c in chan_peers:
            remote(
                bs.at[h, :, group, here(c), :], br.at[h, c_me, :, group, span, :],
                b_send, b_recv.at[g, h, q], chan=c,
            )
        own(
            bs.at[h, :, group, here(c_me), :], br.at[h, c_me, :, group, span, :],
            b_own.at[g, h, q],
        )

    arrived = set()

    def returned(g, n):
        if (g, n) not in arrived:
            arrived.add((g, n))
            from_slabs(tr, g, n, t_recv, t_own)

    def gather(g, n):
        h, q = n // PARTS, n % PARTS
        span = pl.ds(q * piece, piece)
        group = pl.ds(first_of[g], G)
        if g == FAR and n >= BACK_DEPTH:
            returned(g, n - BACK_DEPTH)
        landed(br.at[h, pl.ds(0, C - 1), :, group, span, :], b_recv.at[g, h, q])
        landed(br.at[h, 0, :, group, span, :], b_own.at[g, h, q])

        def body(i, carry):
            s = first_of[g] + i
            base, slope = None, None
            for c in range(C):
                offset = (offs[c, 0:1, :] - 1.0)[None]
                value = br[h, c, :, s, span, :]
                base = value if base is None else base + value
                slope = offset * value if slope is None else slope + offset * value
            ts[h, s, :, 0, span, :] = base * scale
            ts[h, s, :, 1, span, :] = slope * scale
            return carry

        lax.fori_loop(0, G, body, 0)
        to_slabs(ts, tr, g, n, t_send, t_recv, t_own)

    def back_in(h, p):
        returned(FAR, h * PARTS + p)
        returned(NEAR, h * PARTS + p)

        def flip(s, carry):
            for part in range(2):
                tile = tr[h, s, part, :, halved(p), :].reshape(wide, LANES).T
                for jl in range(jper):
                    x_s[jl, pl.ds(al8(kl * s), kl), part * LANES : part * LANES + wide] = tile[
                        kl * jl : kl * (jl + 1), :
                    ]
            return carry

        lax.fori_loop(0, S, flip, 0)

        def body(jl, carry):
            zr, zi = fine(bwd[jper * h + jl], x_s[jl])
            y_s[p, jper * h + jl, :, 0:LANES] = zr
            y_s[p, jper * h + jl, :, LANES : 2 * LANES] = zi
            return carry

        lax.fori_loop(0, jper, body, 0, unroll=2)

    def back_out(p):
        def body(n, carry):
            out = sixteen([get(y_s, p, j, at=8 * n) for j in range(RADIX)], 1)
            for b in range(RADIX):
                xt[b, pl.ds(al8(8 * n), 8), :] = out[b][0]
            return carry

        lax.fori_loop(0, LANES // 8, body, 0)
        per = cols // LANES
        for b in range(RADIX):
            os_[b // per, :, halved(p), LANES * (b % per) : LANES * (b % per + 1)] = (
                xt[b, :, 0:wide].T.reshape(TERMS, half, LANES)
            )
        there = pl.ds(al8(sub * c_me + p * half), half)
        for c in chan_peers:
            remote(os_.at[c, :, halved(p), :], out_hbm.at[:, there, :], o_send, o_recv, chan=c)
        own(os_.at[c_me, :, halved(p), :], out_hbm.at[:, there, :], o_done)

    for n in range(1, 5):
        load(n).wait()
    prep(0, 0, 8)
    load(0).wait()
    load(5).wait()
    landed(offs.at[0], o_own)
    rows_in(0)
    rows_out(0, 0)
    send_rows(FAR, 0)
    send_rows(NEAR, 0)
    rows_in(1)
    rows_out(0, 1)
    send_rows(FAR, 1)
    send_rows(NEAR, 1)
    landed(offs.at[pl.ds(0, C - 1)], f_recv)
    mix(NEAR, 0)
    rows_in(2)
    rows_out(0, 2)
    send_rows(NEAR, 2)
    mix(NEAR, 1)
    mix(FAR, 0)
    send_rows(FAR, 2)
    rows_in(3)
    rows_out(0, 3)
    send_rows(NEAR, 3)
    mix(NEAR, 2)
    rows_out(1, 0)
    mix(NEAR, 3)
    mix(FAR, 1)
    send_rows(FAR, 3)
    rows_out(1, 1)
    prep(1, 0, 4)
    mix(FAR, 2)
    send_rows(FAR, 4)
    send_rows(NEAR, 4)
    prep(1, 4, 8)
    rows_out(1, 2)
    mix(FAR, 3)
    send_rows(FAR, 5)
    send_rows(NEAR, 5)
    rows_out(1, 3)
    mix(NEAR, 4)
    prep(2, 0, 4)
    mix(NEAR, 5)
    mix(FAR, 4)
    send_rows(FAR, 6)
    send_rows(NEAR, 6)
    prep(2, 4, 8)
    column_in(0)
    mix(NEAR, 6)
    column_mid(0, 0, 4)
    mix(FAR, 5)
    send_rows(FAR, 7)
    send_rows(NEAR, 7)
    column_mid(0, 4, 10)
    mix(NEAR, 7)
    column_mid(0, 10, 16)
    column_out(0)
    send_back(FAR, 0)
    mix(FAR, 6)
    send_back(FAR, 1)
    mix(FAR, 7)
    send_back(FAR, 2)
    gather(FAR, 0)
    send_back(FAR, 3)
    gather(FAR, 1)
    send_back(NEAR, 0)
    column_in(1)
    send_back(NEAR, 1)
    column_mid(1, 0, 8)
    gather(FAR, 2)
    column_mid(1, 8, 16)
    gather(FAR, 3)
    column_out(1)
    send_back(FAR, 4)
    gather(NEAR, 0)
    send_back(FAR, 5)
    gather(NEAR, 1)
    send_back(FAR, 6)
    send_back(FAR, 7)
    gather(FAR, 4)
    send_back(NEAR, 2)
    gather(FAR, 5)
    send_back(NEAR, 3)
    back_in(0, 0)
    gather(FAR, 6)
    send_back(NEAR, 4)
    back_in(0, 1)
    gather(FAR, 7)
    send_back(NEAR, 5)
    gather(NEAR, 2)
    send_back(NEAR, 6)
    gather(NEAR, 3)
    send_back(NEAR, 7)
    gather(NEAR, 4)
    back_in(0, 2)
    gather(NEAR, 5)
    back_in(0, 3)
    gather(NEAR, 6)
    back_in(1, 0)
    back_out(0)
    gather(NEAR, 7)
    back_in(1, 1)
    back_out(1)
    back_in(1, 2)
    back_out(2)
    back_in(1, 3)
    back_out(3)

    landed(xr.at[pl.ds(0, C - 1)], x_send)
    landed(offs.at[pl.ds(0, C - 1)], f_send)
    landed(rs.at[:, pl.ds(0, S - 1)], r_send)
    landed(ms.at[:, pl.ds(0, C - 1)], m_send)
    landed(br.at[:, pl.ds(0, C - 1)], b_send)
    landed(ts.at[:, pl.ds(0, S - 1)], t_send)
    landed(os_.at[pl.ds(0, C - 1)], o_send)
    landed(os_.at[pl.ds(0, C - 1)], o_recv)
    landed(os_.at[0], o_done)


def tiled(taylor_models, gridded_vis, uv_weight, freq_ratio, robust_scale):
    C, S = lax.axis_size("chan"), lax.axis_size("slab")
    terms, rows, cols = taylor_models.shape
    sub = rows // C
    U = gridded_vis.shape[2]
    H = U // LANES
    fwd, bwd = fine_tables()
    pu, pv = swap_table(RADIX, U // RADIX), swap_table(RADIX, 16)
    freq = jnp.broadcast_to(freq_ratio[:, None], (8, LANES))
    f32, bf16 = jnp.float32, jnp.bfloat16
    stage = (RADIX, LANES, 2 * LANES)
    slabbed = (H, S, 2, terms, sub, LANES)
    chanbed = (H, C, 2, S, sub, LANES)
    natural = (H, 2, S, rows, LANES)
    V = lambda shape, dtype=f32: pltpu.VMEM(shape, dtype)
    D = pltpu.SemaphoreType.DMA
    anywhere = pl.BlockSpec(memory_space=pl.ANY)
    return pl.pallas_call(
        functools.partial(kernel, C, S),
        out_shape=jax.ShapeDtypeStruct(taylor_models.shape, f32),
        in_specs=[
            anywhere, anywhere, anywhere,
            pl.BlockSpec(memory_space=pltpu.VMEM), pl.BlockSpec(memory_space=pltpu.SMEM),
            anywhere, anywhere, anywhere, anywhere,
        ],
        out_specs=anywhere,
        scratch_shapes=[
            V((C, terms, sub, cols)), V((RADIX, LANES, LANES)), V((HALVES, *stage)), V((H, *stage)),
            V((S, 2, LANES, LANES)), V(slabbed), V(slabbed), V(chanbed), V(natural),
            V(natural), V(chanbed), V(slabbed), V(slabbed), V(stage),
            V((C, terms, sub, cols)), V(fwd.shape, bf16), V(bwd.shape, bf16),
            V(pu.shape, bf16), V(pv.shape, bf16),
            V((3, U, RADIX * LANES), bf16), V((3, H, RADIX, LANES, LANES), bf16),
            V((C, 8, LANES)),
            D((6,)), D(()), D((HALVES,)), D((HALVES,)), D(()), D(()), D(()), D(()), D(()), D(()),
            D(()), D((2, H, PARTS)), D((H, PARTS)),
            D(()), D((H,)), D((H,)),
            D(()), D((2, H, PARTS)), D((2, H, PARTS)),
            D(()), D((2, H, PARTS)), D((H, PARTS)),
        ],
        compiler_params=pltpu.CompilerParams(
            collective_id=0, has_side_effects=True, vmem_limit_bytes=63 * 1024 * 1024
        ),
    )(taylor_models, gridded_vis, uv_weight, freq, robust_scale, fwd, bwd, pu, pv)


HIGHEST = lax.Precision.HIGH


def dft_table(points, direction):
    steps_all = jnp.arange(points, dtype=jnp.int32)
    product = steps_all[:, None] * steps_all[None, :] % points
    angles = product.astype(jnp.float32) * (2.0 * math.pi / points)
    return (jnp.cos(angles), direction * jnp.sin(angles))


def twiddle_table(outer_points, inner_points, direction):
    outer_steps = jnp.arange(outer_points, dtype=jnp.int32)
    inner_steps = jnp.arange(inner_points, dtype=jnp.int32)
    overall = outer_points * inner_points
    product = outer_steps[:, None] * inner_steps[None, :] % overall
    angles = product.astype(jnp.float32) * (2.0 * math.pi / overall)
    return (jnp.cos(angles), direction * jnp.sin(angles))


def complex_product(formula, left_real, left_imag, table_real, table_imag):
    out_real = jnp.einsum(formula, left_real, table_real, precision=HIGHEST) - jnp.einsum(
        formula, left_imag, table_imag, precision=HIGHEST
    )
    out_imag = jnp.einsum(formula, left_real, table_imag, precision=HIGHEST) + jnp.einsum(
        formula, left_imag, table_real, precision=HIGHEST
    )
    return (out_real, out_imag)


def rotate(left_real, left_imag, table_real, table_imag):
    return (
        left_real * table_real - left_imag * table_imag,
        left_real * table_imag + left_imag * table_real,
    )


def general(taylor_models, gridded_vis, uv_weight, freq_ratio, robust_scale):
    inner_count = 128
    PIX = taylor_models.shape[2] * lax.axis_size("chan")
    outer_count = PIX // inner_count
    chans = lax.axis_size("chan")
    slabs = lax.axis_size("slab")
    rows = taylor_models.shape[1]
    cols = taylor_models.shape[2]
    sub = rows // chans
    col_count = PIX // slabs
    outer_cos, outer_sin = dft_table(outer_count, -1.0)
    inner_cos, inner_sin = dft_table(inner_count, -1.0)
    twist_cos, twist_sin = twiddle_table(outer_count, inner_count, -1.0)
    offsets = lax.all_gather(freq_ratio, "chan", axis=0, tiled=True) - 1.0

    pieces = taylor_models.reshape(TERMS, chans, sub, cols).transpose(1, 0, 2, 3)
    pieces = lax.all_to_all(pieces, "chan", split_axis=0, concat_axis=0, tiled=True)
    layered = pieces.transpose(1, 2, 0, 3).reshape(TERMS * sub, outer_count, inner_count)
    part_real = jnp.einsum("yba,jb->yja", layered, outer_cos, precision=HIGHEST)
    part_imag = jnp.einsum("yba,jb->yja", layered, outer_sin, precision=HIGHEST)
    turned_real, turned_imag = rotate(part_real, part_imag, twist_cos, twist_sin)
    spec_real, spec_imag = complex_product(
        "yja,ka->kjy", turned_real, turned_imag, inner_cos, inner_sin
    )
    outgoing = jnp.stack(
        [
            spec_real.reshape(slabs, col_count, TERMS * sub),
            spec_imag.reshape(slabs, col_count, TERMS * sub),
        ],
        axis=1,
    )
    arrived = lax.all_to_all(outgoing, "slab", split_axis=0, concat_axis=0, tiled=True)
    arrived = arrived.reshape(slabs, 2, col_count, TERMS, sub)
    arrived = arrived.transpose(3, 1, 2, 0, 4).reshape(TERMS, 2, col_count, slabs * sub)
    mixed = arrived[0][None] + offsets[:, None, None, None] * arrived[1][None]
    mixed = lax.all_to_all(mixed, "chan", split_axis=0, concat_axis=0, tiled=True)
    columns = mixed.reshape(chans, 2, col_count, slabs, sub).transpose(1, 2, 3, 0, 4)
    layered_cols = columns.reshape(2, col_count, outer_count, inner_count)
    part_real, part_imag = complex_product(
        "uba,jb->uja", layered_cols[0], layered_cols[1], outer_cos, outer_sin
    )
    turned_real, turned_imag = rotate(part_real, part_imag, twist_cos, twist_sin)
    freq_real, freq_imag = complex_product(
        "uja,ka->ujk", turned_real, turned_imag, inner_cos, inner_sin
    )
    freq_real = freq_real / PIX
    freq_imag = freq_imag / PIX
    weight = (
        uv_weight[0]
        .astype(jnp.float32)
        .reshape(col_count, inner_count, outer_count)
        .transpose(0, 2, 1)
    )
    visible = (
        gridded_vis[0]
        .astype(jnp.float32)
        .reshape(2, col_count, inner_count, outer_count)
        .transpose(0, 1, 3, 2)
    )
    delta_real = visible[0] - weight * freq_real
    delta_imag = visible[1] - weight * freq_imag
    robust = 1.0 / (1.0 + robust_scale[0] * (delta_real * delta_real + delta_imag * delta_imag))
    weighted_real = robust * delta_real
    weighted_imag = robust * delta_imag
    back_real, back_imag = complex_product(
        "ujk,ak->uja", weighted_real, weighted_imag, inner_cos, -inner_sin
    )
    back_real, back_imag = rotate(back_real, back_imag, twist_cos, -twist_sin)
    back_real, back_imag = complex_product(
        "uja,bj->uba", back_real, back_imag, outer_cos, -outer_sin
    )
    back = jnp.stack([back_real, back_imag]).reshape(2, col_count, slabs, chans, sub)
    back = back.transpose(3, 0, 1, 2, 4).reshape(chans, 2, col_count, slabs * sub)
    back = lax.all_to_all(back, "chan", split_axis=0, concat_axis=0, tiled=True)
    total = jnp.stack(
        [jnp.sum(back * offsets[:, None, None, None] ** t, axis=0) for t in range(TERMS)]
    )
    total = total.reshape(TERMS, 2, col_count, slabs, sub).transpose(3, 1, 2, 0, 4)
    total = total.reshape(slabs, 2, col_count, TERMS * sub)
    total = lax.all_to_all(total, "slab", split_axis=0, concat_axis=0, tiled=True)
    layered_rows = total.transpose(1, 0, 2, 3).reshape(2, inner_count, outer_count, TERMS * sub)
    last_real, last_imag = complex_product(
        "kjy,ak->ajy", layered_rows[0], layered_rows[1], inner_cos, -inner_sin
    )
    last_real, last_imag = rotate(
        last_real, last_imag, twist_cos.T[:, :, None], -twist_sin.T[:, :, None]
    )
    image_out = jnp.einsum("ajy,bj->yba", last_real, outer_cos, precision=HIGHEST) + jnp.einsum(
        "ajy,bj->yba", last_imag, outer_sin, precision=HIGHEST
    )
    image_out = image_out.reshape(TERMS, sub, chans, cols).transpose(2, 0, 1, 3) / PIX
    tiles = lax.all_to_all(image_out, "chan", split_axis=0, concat_axis=0, tiled=True)
    return tiles.transpose(1, 0, 2, 3).reshape(TERMS, rows, cols)


def local(taylor_models, gridded_vis, uv_weight, freq_ratio, robust_scale):
    C, S = lax.axis_size("chan"), lax.axis_size("slab")
    terms, rows, cols = taylor_models.shape
    pix, sub, U = cols * C, rows // C, gridded_vis.shape[2]
    fits = (
        terms == TERMS
        and pix == RADIX * LANES
        and rows * S == pix
        and rows % LANES == 0
        and cols % LANES == 0
        and terms * sub == LANES
        and sub % (8 * PARTS) == 0
        and LANES % (8 * S) == 0
        and S % 2 == 0
        and PARTS == HALVES
        and U == 2 * LANES
    )
    form = tiled if fits else general
    return form(taylor_models, gridded_vis, uv_weight, freq_ratio, robust_scale)


def solution(mesh):
    placed = (
        P(None, "slab", "chan"),
        P("chan", None, "slab", None),
        P("chan", "slab", None),
        P("chan"),
        P("chan"),
    )
    return jax.shard_map(
        local, mesh=mesh, in_specs=placed, out_specs=P(None, "slab", "chan"), check_vma=False
    )
```

```python
import functools
import math

import jax
import jax.numpy as jnp
import numpy as np
from jax import lax
from jax.experimental import pallas as pl
from jax.experimental.pallas import tpu as pltpu
from jax.sharding import PartitionSpec as P

MESH = pl.DeviceIdType.MESH
TERMS = 2
RADIX = 16
LANES = 128
PARTS = 4
NEAR, FAR = 0, 1
BACK_DEPTH = 8
HALVES = 4


def fine_tables():
    points = RADIX * LANES
    j = np.arange(RADIX)[:, None, None]
    k = np.arange(LANES)[None, :, None]
    a = np.arange(LANES)[None, None, :]
    angle = 2.0 * np.pi / points * ((a * (RADIX * k + j)) % points)
    cos, sin = np.cos(angle), -np.sin(angle)

    def halves(real, imag):
        table = np.concatenate([real, imag], axis=1).astype(np.float32)
        high = table.astype(jnp.bfloat16)
        low = (table - high.astype(np.float32)).astype(jnp.bfloat16)
        return np.concatenate([high, low], axis=2)

    flip = lambda t: t.transpose(0, 2, 1)
    return halves(cos, sin), halves(flip(cos), -flip(sin))


def swap_table(outer, inner):
    size = outer * inner
    table = np.zeros((size, size), np.float32)
    rows = np.arange(size)
    table[rows, (rows % inner) * outer + rows // inner] = 1.0
    return table.astype(jnp.bfloat16)


def plus(a, b):
    if a is None:
        return b
    return a if b is None else a + b


def minus(a, b):
    if b is None:
        return a
    return -b if a is None else a - b


def times(a, s):
    return None if a is None or s == 0.0 else a * s


def cadd(a, b):
    return plus(a[0], b[0]), plus(a[1], b[1])


def csub(a, b):
    return minus(a[0], b[0]), minus(a[1], b[1])


def turn(a, sign):
    if sign > 0:
        return minus(None, a[1]) if a[1] is not None else None, a[0]
    return a[1], minus(None, a[0]) if a[0] is not None else None


def ctwist(a, step, sign):
    step %= RADIX
    if step == 0:
        return a
    if step == 4:
        return turn(a, sign)
    c, s = math.cos(2 * math.pi * step / RADIX), sign * math.sin(2 * math.pi * step / RADIX)
    if step % 8 == 2:
        return times(minus(a[0], times(a[1], sign)), c), times(plus(times(a[0], sign), a[1]), c)
    return minus(times(a[0], c), times(a[1], s)), plus(times(a[0], s), times(a[1], c))


def four(a, b, c, d, sign):
    t0, t1, t2, t3 = cadd(a, c), csub(a, c), cadd(b, d), turn(csub(b, d), sign)
    return cadd(t0, t2), cadd(t1, t3), csub(t0, t2), csub(t1, t3)


def sixteen(x, sign):
    mid = [four(x[n], x[4 + n], x[8 + n], x[12 + n], sign) for n in range(4)]
    out = [None] * RADIX
    for k in range(4):
        tw = [ctwist(mid[n][k], n * k, sign) for n in range(4)]
        for q, y in enumerate(four(*tw, sign)):
            out[k + 4 * q] = y
    return out


def fine(table, x):
    high = x.astype(jnp.bfloat16)
    low = (x - high.astype(jnp.float32)).astype(jnp.bfloat16)
    t_high, t_low = table[:, :LANES], table[:, LANES:]
    left = jnp.concatenate(
        [jnp.concatenate([t_high, t_high], axis=1), jnp.concatenate([t_low, t_low], axis=1)], axis=0
    )
    out = jnp.dot(left, jnp.concatenate([high, low], axis=0), preferred_element_type=jnp.float32)
    out = out[: 2 * LANES] + out[2 * LANES :]
    n = x.shape[1] // 2
    real = out[:LANES, :n] - out[LANES:, n:]
    imag = out[:LANES, n:] + out[LANES:, :n]
    return real, imag


def put(ref, *index, at, value):
    for part in range(2):
        v = value[part]
        if v is None:
            v = jnp.zeros((8, LANES), jnp.float32)
        ref[(*index, pl.ds(al8(at), 8), pl.ds(part * LANES, LANES))] = v


def get(ref, *index, at):
    return tuple(ref[(*index, pl.ds(al8(at), 8), pl.ds(part * LANES, LANES))] for part in range(2))


def al8(i):
    return pl.multiple_of(i, 8)


def kernel(
    C, S,
    x_hbm, vis_hbm, wt_hbm, freq_ref, rob_ref, fwd_hbm, bwd_hbm, pu_hbm, pv_hbm,
    out_hbm,
    xr, xt, y_s, z_s, w_s, rs, rr, ms, mr, bs, br, ts, tr, x_s, os_, fwd, bwd, pu, pv,
    raw, vt, offs, mine,
    load_sem, x_send, x_recv, x_own, o_send, o_recv, o_own, o_done, f_send, f_recv,
    r_send, r_recv, r_own, m_send, m_recv, m_own, b_send, b_recv, b_own, t_send, t_recv, t_own,
):
    H = rs.shape[0]
    sub = x_hbm.shape[1] // C
    rows, cols = x_hbm.shape[1], x_hbm.shape[2]
    jper = RADIX // H
    kl = LANES // S
    piece = sub // PARTS
    scale = 1.0 / (RADIX * LANES)
    c_me, s_me = lax.axis_index("chan"), lax.axis_index("slab")
    chan_peers = [lax.rem(c_me + d, C) for d in range(1, C)]
    if C == 4:
        chan_peers = [3 - c_me, c_me + 1 - 2 * lax.rem(c_me, 2), lax.rem(c_me + 2, 4)]
    G = S // 2
    low = s_me // G * G
    first_of = (low, G - low)
    slab_peers = (
        [low + lax.rem(s_me + d, G) for d in range(1, G)],
        [G - low + lax.rem(s_me + d, G) for d in range(G)],
    )

    def load(n):
        source, target = (
            (fwd_hbm, fwd),
            (vis_hbm.at[0], raw.at[pl.ds(0, 2)]),
            (wt_hbm, raw.at[pl.ds(2, 1)]),
            (pu_hbm, pu),
            (pv_hbm, pv),
            (bwd_hbm, bwd),
        )[n]
        return pltpu.make_async_copy(source, target, load_sem.at[n])

    def remote(src, dst, send, recv, **where):
        pltpu.make_async_remote_copy(
            src_ref=src, dst_ref=dst, send_sem=send, recv_sem=recv,
            device_id=where, device_id_type=MESH,
        ).start()

    def own(src, dst, sem):
        pltpu.make_async_copy(src, dst, sem).start()

    def landed(ref, sem):
        pltpu.make_async_copy(ref, ref, sem).wait()

    half = sub // HALVES
    halved = lambda p: pl.ds(p * half, half)
    wide = TERMS * half

    mine[...] = jnp.full(mine.shape, freq_ref[0] - 1.0, jnp.float32)
    barrier = pltpu.get_barrier_semaphore()
    for c in chan_peers:
        pl.semaphore_signal(barrier, inc=1, device_id={"chan": c}, device_id_type=MESH)
    for s in slab_peers[NEAR] + slab_peers[FAR]:
        pl.semaphore_signal(barrier, inc=1, device_id={"slab": s}, device_id_type=MESH)
    for p in range(HALVES):
        own(
            x_hbm.at[:, pl.ds(al8(sub * c_me + p * half), half), :],
            xr.at[c_me, :, halved(p), :], x_own.at[p],
        )
    for n in range(6):
        load(n).start()
    pl.semaphore_wait(barrier, C + S - 2)

    own(mine, offs.at[c_me], o_own)
    for c in chan_peers:
        remote(mine, offs.at[c_me], f_send, f_recv, chan=c)

    def send_tiles(p):
        for c in chan_peers:
            remote(
                x_hbm.at[:, pl.ds(al8(sub * c + p * half), half), :],
                xr.at[c_me, :, halved(p), :], x_send, x_recv.at[p], chan=c,
            )

    def prep(which, first, last):
        def body(m, carry):
            block = raw[which, :, pl.ds(pl.multiple_of(m * 256, 256), 256)]
            turned = jnp.dot(pu[...], block, preferred_element_type=jnp.float32)
            flipped = lax.dot_general(
                pv[...], turned.astype(jnp.bfloat16), (((1,), (1,)), ((), ())),
                preferred_element_type=jnp.float32,
            ).astype(jnp.bfloat16)
            for h in range(H):
                for j in range(RADIX):
                    vt[which, h, j, pl.ds(pl.multiple_of(16 * m, 16), 16), :] = flipped[
                        16 * j : 16 * j + 16, LANES * h : LANES * (h + 1)
                    ]
            return carry

        lax.fori_loop(first, last, body, 0)

    def rows_in(p):
        landed(xr.at[pl.ds(0, C - 1), :, halved(p), :], x_recv.at[p])
        landed(xr.at[0, :, halved(p), :], x_own.at[p])
        per = cols // LANES
        for b in range(RADIX):
            tile = xr[b // per, :, halved(p), LANES * (b % per) : LANES * (b % per + 1)]
            xt[b, :, 0:wide] = tile.reshape(wide, LANES).T

        def body(n, carry):
            out = sixteen([(xt[b, pl.ds(al8(8 * n), 8), :], None) for b in range(RADIX)], -1)
            for j in range(RADIX):
                put(y_s, p, j, at=8 * n, value=out[j])
            return carry

        lax.fori_loop(0, LANES // 8, body, 0)

    def rows_out(h, p):
        def body(jl, carry):
            z = fine(fwd[jper * h + jl], y_s[p, jper * h + jl])
            for s in range(S):
                for part in range(2):
                    w_s[s, part, pl.ds(al8(kl * jl), kl), :] = z[part][kl * s : kl * (s + 1), :]
            return carry

        lax.fori_loop(0, jper, body, 0, unroll=4)

        def flip(s, carry):
            for part in range(2):
                rs[h, s, part, :, halved(p), :] = w_s[s, part, :, 0:wide].T.reshape(TERMS, half, LANES)
            return carry

        lax.fori_loop(0, S, flip, 0, unroll=2)

    def to_slabs(source, target, g, n, send, recv, done):
        h, q = n // PARTS, n % PARTS
        span = pl.ds(q * piece, piece)
        for s in slab_peers[g]:
            remote(
                source.at[h, s, :, :, span, :], target.at[h, s_me, :, :, span, :],
                send, recv.at[g, h, q], slab=s,
            )
        if g == NEAR:
            own(
                source.at[h, s_me, :, :, span, :], target.at[h, s_me, :, :, span, :],
                done.at[h, q],
            )

    def from_slabs(target, g, n, recv, done):
        h, q = n // PARTS, n % PARTS
        span = pl.ds(q * piece, piece)
        landed(target.at[h, pl.ds(0, len(slab_peers[g])), :, :, span, :], recv.at[g, h, q])
        if g == NEAR:
            landed(target.at[h, 0, :, :, span, :], done.at[h, q])

    def send_rows(g, n):
        to_slabs(rs, rr, g, n, r_send, r_recv, r_own)

    def mix(g, n):
        h, q = n // PARTS, n % PARTS
        span = pl.ds(q * piece, piece)
        from_slabs(rr, g, n, r_recv, r_own)

        def body(i, carry):
            s = first_of[g] + i
            base = rr[h, s, :, 0, span, :] * scale
            slope = rr[h, s, :, 1, span, :] * scale
            for c in range(C):
                offset = offs[c, 0:1, :]
                ms[h, c, :, s, span, :] = base + offset[None] * slope
            return carry

        lax.fori_loop(0, G, body, 0)
        there = pl.ds(al8(sub * c_me + q * piece), piece)
        group = pl.ds(first_of[g], G)
        for c in chan_peers:
            remote(
                ms.at[h, c, :, group, span, :], mr.at[h, :, group, there, :],
                m_send, m_recv.at[h], chan=c,
            )
        own(ms.at[h, c_me, :, group, span, :], mr.at[h, :, group, there, :], m_own.at[h])

    def column_in(h):
        landed(ms.at[h, pl.ds(0, C - 1)], m_recv.at[h])
        landed(ms.at[h, 0], m_own.at[h])

        def body(n, carry):
            at = 8 * n
            x = []
            for b in range(RADIX):
                s, row = LANES * b // rows, LANES * b % rows
                x.append(tuple(mr[h, part, s, pl.ds(al8(row + at), 8), :] for part in range(2)))
            out = sixteen(x, -1)
            for j in range(RADIX):
                put(y_s, h, j, at=at, value=out[j])
            return carry

        lax.fori_loop(0, LANES // 8, body, 0)

    def column_mid(h, first, last):
        def body(j, carry):
            zr, zi = fine(fwd[j], y_s[h, j])
            weight = vt[2, h, j].astype(jnp.float32)
            real = vt[0, h, j].astype(jnp.float32) - weight * zr
            imag = vt[1, h, j].astype(jnp.float32) - weight * zi
            robust = 1.0 / (1.0 + rob_ref[0] * (real * real + imag * imag))
            zr, zi = fine(bwd[j], jnp.concatenate([robust * real, robust * imag], axis=1))
            z_s[h, j, :, 0:LANES] = zr
            z_s[h, j, :, LANES : 2 * LANES] = zi
            return carry

        lax.fori_loop(first, last, body, 0, unroll=2)

    def column_out(h):
        def body(n, carry):
            out = sixteen([get(z_s, h, j, at=8 * n) for j in range(RADIX)], 1)
            for b in range(RADIX):
                s, row = LANES * b // rows, LANES * b % rows
                for part in range(2):
                    bs[h, part, s, pl.ds(al8(row + 8 * n), 8), :] = out[b][part]
            return carry

        lax.fori_loop(0, LANES // 8, body, 0)

    def send_back(g, n):
        h, q = n // PARTS, n % PARTS
        span = pl.ds(q * piece, piece)
        group = pl.ds(first_of[g], G)
        here = lambda c: pl.ds(al8(sub * c + q * piece), piece)
        for c in chan_peers:
            remote(
                bs.at[h, :, group, here(c), :], br.at[h, c_me, :, group, span, :],
                b_send, b_recv.at[g, h, q], chan=c,
            )
        own(
            bs.at[h, :, group, here(c_me), :], br.at[h, c_me, :, group, span, :],
            b_own.at[g, h, q],
        )

    arrived = set()

    def returned(g, n):
        if (g, n) not in arrived:
            arrived.add((g, n))
            from_slabs(tr, g, n, t_recv, t_own)

    def gather(g, n):
        h, q = n // PARTS, n % PARTS
        span = pl.ds(q * piece, piece)
        group = pl.ds(first_of[g], G)
        if g == FAR and n >= BACK_DEPTH:
            returned(g, n - BACK_DEPTH)
        landed(br.at[h, pl.ds(0, C - 1), :, group, span, :], b_recv.at[g, h, q])
        landed(br.at[h, 0, :, group, span, :], b_own.at[g, h, q])

        def body(i, carry):
            s = first_of[g] + i
            base, slope = None, None
            for c in range(C):
                offset = (offs[c, 0:1, :])[None]
                value = br[h, c, :, s, span, :]
                base = value if base is None else base + value
                slope = offset * value if slope is None else slope + offset * value
            ts[h, s, :, 0, span, :] = base * scale
            ts[h, s, :, 1, span, :] = slope * scale
            return carry

        lax.fori_loop(0, G, body, 0)
        to_slabs(ts, tr, g, n, t_send, t_recv, t_own)

    def back_in(h, p):
        returned(FAR, h * PARTS + p)
        returned(NEAR, h * PARTS + p)

        def flip(s, carry):
            for part in range(2):
                tile = tr[h, s, part, :, halved(p), :].reshape(wide, LANES).T
                for jl in range(jper):
                    x_s[jl, pl.ds(al8(kl * s), kl), part * LANES : part * LANES + wide] = tile[
                        kl * jl : kl * (jl + 1), :
                    ]
            return carry

        lax.fori_loop(0, S, flip, 0, unroll=2)

        def body(jl, carry):
            zr, zi = fine(bwd[jper * h + jl], x_s[jl])
            y_s[p, jper * h + jl, :, 0:LANES] = zr
            y_s[p, jper * h + jl, :, LANES : 2 * LANES] = zi
            return carry

        lax.fori_loop(0, jper, body, 0, unroll=4)

    def back_out(p):
        def body(n, carry):
            out = sixteen([get(y_s, p, j, at=8 * n) for j in range(RADIX)], 1)
            for b in range(RADIX):
                xt[b, pl.ds(al8(8 * n), 8), :] = out[b][0]
            return carry

        lax.fori_loop(0, LANES // 8, body, 0)
        per = cols // LANES
        for b in range(RADIX):
            os_[b // per, :, halved(p), LANES * (b % per) : LANES * (b % per + 1)] = (
                xt[b, :, 0:wide].T.reshape(TERMS, half, LANES)
            )
        there = pl.ds(al8(sub * c_me + p * half), half)
        for c in chan_peers:
            remote(os_.at[c, :, halved(p), :], out_hbm.at[:, there, :], o_send, o_recv, chan=c)
        own(os_.at[c_me, :, halved(p), :], out_hbm.at[:, there, :], o_done)

    for p in range(HALVES):
        send_tiles(p)
    for n in range(1, 5):
        load(n).wait()
    prep(0, 0, 8)
    load(0).wait()
    load(5).wait()
    landed(offs.at[0], o_own)
    rows_in(0)
    rows_out(0, 0)
    send_rows(NEAR, 0)
    send_rows(FAR, 0)
    rows_in(1)
    rows_out(0, 1)
    send_rows(NEAR, 1)
    send_rows(FAR, 1)
    landed(offs.at[pl.ds(0, C - 1)], f_recv)
    mix(NEAR, 0)
    rows_in(2)
    rows_out(0, 2)
    send_rows(NEAR, 2)
    mix(NEAR, 1)
    rows_in(3)
    rows_out(0, 3)
    send_rows(NEAR, 3)
    mix(FAR, 0)
    send_rows(FAR, 2)
    mix(NEAR, 2)
    rows_out(1, 0)
    mix(NEAR, 3)
    prep(1, 0, 4)
    mix(FAR, 1)
    send_rows(FAR, 3)
    rows_out(1, 1)
    prep(1, 4, 8)
    rows_out(1, 2)
    mix(FAR, 2)
    send_rows(NEAR, 4)
    send_rows(FAR, 4)
    rows_out(1, 3)
    prep(2, 0, 4)
    mix(FAR, 3)
    send_rows(NEAR, 5)
    send_rows(FAR, 5)
    mix(NEAR, 4)
    prep(2, 4, 8)
    mix(NEAR, 5)
    column_in(0)
    mix(FAR, 4)
    send_rows(NEAR, 6)
    send_rows(FAR, 6)
    column_mid(0, 0, 10)
    mix(FAR, 5)
    send_rows(NEAR, 7)
    send_rows(FAR, 7)
    column_mid(0, 10, 16)
    column_out(0)
    send_back(FAR, 0)
    mix(NEAR, 6)
    send_back(FAR, 1)
    mix(FAR, 6)
    send_back(FAR, 2)
    mix(NEAR, 7)
    gather(FAR, 0)
    mix(FAR, 7)
    send_back(FAR, 3)
    gather(FAR, 1)
    send_back(NEAR, 0)
    gather(FAR, 2)
    send_back(NEAR, 1)
    column_in(1)
    column_mid(1, 0, 8)
    gather(FAR, 3)
    column_mid(1, 8, 16)
    column_out(1)
    send_back(FAR, 4)
    send_back(FAR, 5)
    gather(NEAR, 0)
    gather(NEAR, 1)
    send_back(FAR, 6)
    send_back(FAR, 7)
    gather(FAR, 4)
    send_back(NEAR, 4)
    gather(FAR, 5)
    send_back(NEAR, 5)
    back_in(0, 0)
    send_back(NEAR, 2)
    gather(FAR, 6)
    send_back(NEAR, 6)
    back_in(0, 1)
    gather(FAR, 7)
    send_back(NEAR, 3)
    send_back(NEAR, 7)
    gather(NEAR, 4)
    gather(NEAR, 5)
    back_in(1, 0)
    back_out(0)
    gather(NEAR, 2)
    back_in(1, 1)
    back_out(1)
    gather(NEAR, 6)
    back_in(0, 2)
    gather(NEAR, 3)
    back_in(1, 2)
    back_out(2)
    gather(NEAR, 7)
    back_in(0, 3)
    back_in(1, 3)
    back_out(3)

    landed(xr.at[pl.ds(0, C - 1)], x_send)
    landed(offs.at[pl.ds(0, C - 1)], f_send)
    landed(rs.at[:, pl.ds(0, S - 1)], r_send)
    landed(ms.at[:, pl.ds(0, C - 1)], m_send)
    landed(br.at[:, pl.ds(0, C - 1)], b_send)
    landed(ts.at[:, pl.ds(0, S - 1)], t_send)
    landed(os_.at[pl.ds(0, C - 1)], o_send)
    landed(os_.at[pl.ds(0, C - 1)], o_recv)
    landed(os_.at[0], o_done)


def tiled(taylor_models, gridded_vis, uv_weight, freq_ratio, robust_scale):
    C, S = lax.axis_size("chan"), lax.axis_size("slab")
    terms, rows, cols = taylor_models.shape
    sub = rows // C
    U = gridded_vis.shape[2]
    H = U // LANES
    fwd, bwd = fine_tables()
    pu, pv = swap_table(RADIX, U // RADIX), swap_table(RADIX, 16)
    f32, bf16 = jnp.float32, jnp.bfloat16
    stage = (RADIX, LANES, 2 * LANES)
    slabbed = (H, S, 2, terms, sub, LANES)
    chanbed = (H, C, 2, S, sub, LANES)
    natural = (H, 2, S, rows, LANES)
    V = lambda shape, dtype=f32: pltpu.VMEM(shape, dtype)
    D = pltpu.SemaphoreType.DMA
    anywhere = pl.BlockSpec(memory_space=pl.ANY)
    return pl.pallas_call(
        functools.partial(kernel, C, S),
        out_shape=jax.ShapeDtypeStruct(taylor_models.shape, f32),
        in_specs=[
            anywhere, anywhere, anywhere,
            pl.BlockSpec(memory_space=pltpu.SMEM), pl.BlockSpec(memory_space=pltpu.SMEM),
            anywhere, anywhere, anywhere, anywhere,
        ],
        out_specs=anywhere,
        scratch_shapes=[
            V((C, terms, sub, cols)), V((RADIX, LANES, LANES)), V((HALVES, *stage)), V((H, *stage)),
            V((S, 2, LANES, LANES)), V(slabbed), V(slabbed), V(chanbed), V(natural),
            V(natural), V(chanbed), V(slabbed), V(slabbed), V((RADIX // H, LANES, 2 * LANES)),
            V((C, terms, sub, cols)), V(fwd.shape, bf16), V(bwd.shape, bf16),
            V(pu.shape, bf16), V(pv.shape, bf16),
            V((3, U, RADIX * LANES), bf16), V((3, H, RADIX, LANES, LANES), bf16),
            V((C, 8, LANES)), V((8, LANES)),
            D((6,)), D(()), D((HALVES,)), D((HALVES,)), D(()), D(()), D(()), D(()), D(()), D(()),
            D(()), D((2, H, PARTS)), D((H, PARTS)),
            D(()), D((H,)), D((H,)),
            D(()), D((2, H, PARTS)), D((2, H, PARTS)),
            D(()), D((2, H, PARTS)), D((H, PARTS)),
        ],
        compiler_params=pltpu.CompilerParams(
            collective_id=0, has_side_effects=True, vmem_limit_bytes=63 * 1024 * 1024
        ),
    )(taylor_models, gridded_vis, uv_weight, freq_ratio, robust_scale, fwd, bwd, pu, pv)


HIGHEST = lax.Precision.HIGH


def dft_table(points, direction):
    steps_all = jnp.arange(points, dtype=jnp.int32)
    product = steps_all[:, None] * steps_all[None, :] % points
    angles = product.astype(jnp.float32) * (2.0 * math.pi / points)
    return (jnp.cos(angles), direction * jnp.sin(angles))


def twiddle_table(outer_points, inner_points, direction):
    outer_steps = jnp.arange(outer_points, dtype=jnp.int32)
    inner_steps = jnp.arange(inner_points, dtype=jnp.int32)
    overall = outer_points * inner_points
    product = outer_steps[:, None] * inner_steps[None, :] % overall
    angles = product.astype(jnp.float32) * (2.0 * math.pi / overall)
    return (jnp.cos(angles), direction * jnp.sin(angles))


def complex_product(formula, left_real, left_imag, table_real, table_imag):
    out_real = jnp.einsum(formula, left_real, table_real, precision=HIGHEST) - jnp.einsum(
        formula, left_imag, table_imag, precision=HIGHEST
    )
    out_imag = jnp.einsum(formula, left_real, table_imag, precision=HIGHEST) + jnp.einsum(
        formula, left_imag, table_real, precision=HIGHEST
    )
    return (out_real, out_imag)


def rotate(left_real, left_imag, table_real, table_imag):
    return (
        left_real * table_real - left_imag * table_imag,
        left_real * table_imag + left_imag * table_real,
    )


def general(taylor_models, gridded_vis, uv_weight, freq_ratio, robust_scale):
    inner_count = 128
    PIX = taylor_models.shape[2] * lax.axis_size("chan")
    outer_count = PIX // inner_count
    chans = lax.axis_size("chan")
    slabs = lax.axis_size("slab")
    rows = taylor_models.shape[1]
    cols = taylor_models.shape[2]
    sub = rows // chans
    col_count = PIX // slabs
    outer_cos, outer_sin = dft_table(outer_count, -1.0)
    inner_cos, inner_sin = dft_table(inner_count, -1.0)
    twist_cos, twist_sin = twiddle_table(outer_count, inner_count, -1.0)
    offsets = lax.all_gather(freq_ratio, "chan", axis=0, tiled=True) - 1.0

    pieces = taylor_models.reshape(TERMS, chans, sub, cols).transpose(1, 0, 2, 3)
    pieces = lax.all_to_all(pieces, "chan", split_axis=0, concat_axis=0, tiled=True)
    layered = pieces.transpose(1, 2, 0, 3).reshape(TERMS * sub, outer_count, inner_count)
    part_real = jnp.einsum("yba,jb->yja", layered, outer_cos, precision=HIGHEST)
    part_imag = jnp.einsum("yba,jb->yja", layered, outer_sin, precision=HIGHEST)
    turned_real, turned_imag = rotate(part_real, part_imag, twist_cos, twist_sin)
    spec_real, spec_imag = complex_product(
        "yja,ka->kjy", turned_real, turned_imag, inner_cos, inner_sin
    )
    outgoing = jnp.stack(
        [
            spec_real.reshape(slabs, col_count, TERMS * sub),
            spec_imag.reshape(slabs, col_count, TERMS * sub),
        ],
        axis=1,
    )
    arrived = lax.all_to_all(outgoing, "slab", split_axis=0, concat_axis=0, tiled=True)
    arrived = arrived.reshape(slabs, 2, col_count, TERMS, sub)
    arrived = arrived.transpose(3, 1, 2, 0, 4).reshape(TERMS, 2, col_count, slabs * sub)
    mixed = arrived[0][None] + offsets[:, None, None, None] * arrived[1][None]
    mixed = lax.all_to_all(mixed, "chan", split_axis=0, concat_axis=0, tiled=True)
    columns = mixed.reshape(chans, 2, col_count, slabs, sub).transpose(1, 2, 3, 0, 4)
    layered_cols = columns.reshape(2, col_count, outer_count, inner_count)
    part_real, part_imag = complex_product(
        "uba,jb->uja", layered_cols[0], layered_cols[1], outer_cos, outer_sin
    )
    turned_real, turned_imag = rotate(part_real, part_imag, twist_cos, twist_sin)
    freq_real, freq_imag = complex_product(
        "uja,ka->ujk", turned_real, turned_imag, inner_cos, inner_sin
    )
    freq_real = freq_real / PIX
    freq_imag = freq_imag / PIX
    weight = (
        uv_weight[0]
        .astype(jnp.float32)
        .reshape(col_count, inner_count, outer_count)
        .transpose(0, 2, 1)
    )
    visible = (
        gridded_vis[0]
        .astype(jnp.float32)
        .reshape(2, col_count, inner_count, outer_count)
        .transpose(0, 1, 3, 2)
    )
    delta_real = visible[0] - weight * freq_real
    delta_imag = visible[1] - weight * freq_imag
    robust = 1.0 / (1.0 + robust_scale[0] * (delta_real * delta_real + delta_imag * delta_imag))
    weighted_real = robust * delta_real
    weighted_imag = robust * delta_imag
    back_real, back_imag = complex_product(
        "ujk,ak->uja", weighted_real, weighted_imag, inner_cos, -inner_sin
    )
    back_real, back_imag = rotate(back_real, back_imag, twist_cos, -twist_sin)
    back_real, back_imag = complex_product(
        "uja,bj->uba", back_real, back_imag, outer_cos, -outer_sin
    )
    back = jnp.stack([back_real, back_imag]).reshape(2, col_count, slabs, chans, sub)
    back = back.transpose(3, 0, 1, 2, 4).reshape(chans, 2, col_count, slabs * sub)
    back = lax.all_to_all(back, "chan", split_axis=0, concat_axis=0, tiled=True)
    total = jnp.stack(
        [jnp.sum(back * offsets[:, None, None, None] ** t, axis=0) for t in range(TERMS)]
    )
    total = total.reshape(TERMS, 2, col_count, slabs, sub).transpose(3, 1, 2, 0, 4)
    total = total.reshape(slabs, 2, col_count, TERMS * sub)
    total = lax.all_to_all(total, "slab", split_axis=0, concat_axis=0, tiled=True)
    layered_rows = total.transpose(1, 0, 2, 3).reshape(2, inner_count, outer_count, TERMS * sub)
    last_real, last_imag = complex_product(
        "kjy,ak->ajy", layered_rows[0], layered_rows[1], inner_cos, -inner_sin
    )
    last_real, last_imag = rotate(
        last_real, last_imag, twist_cos.T[:, :, None], -twist_sin.T[:, :, None]
    )
    image_out = jnp.einsum("ajy,bj->yba", last_real, outer_cos, precision=HIGHEST) + jnp.einsum(
        "ajy,bj->yba", last_imag, outer_sin, precision=HIGHEST
    )
    image_out = image_out.reshape(TERMS, sub, chans, cols).transpose(2, 0, 1, 3) / PIX
    tiles = lax.all_to_all(image_out, "chan", split_axis=0, concat_axis=0, tiled=True)
    return tiles.transpose(1, 0, 2, 3).reshape(TERMS, rows, cols)


def local(taylor_models, gridded_vis, uv_weight, freq_ratio, robust_scale):
    C, S = lax.axis_size("chan"), lax.axis_size("slab")
    terms, rows, cols = taylor_models.shape
    pix, sub, U = cols * C, rows // C, gridded_vis.shape[2]
    fits = (
        terms == TERMS
        and pix == RADIX * LANES
        and rows * S == pix
        and rows % LANES == 0
        and cols % LANES == 0
        and terms * sub == LANES
        and sub % (8 * PARTS) == 0
        and LANES % (8 * S) == 0
        and S % 2 == 0
        and PARTS == HALVES
        and U == 2 * LANES
    )
    form = tiled if fits else general
    return form(taylor_models, gridded_vis, uv_weight, freq_ratio, robust_scale)


def solution(mesh):
    placed = (
        P(None, "slab", "chan"),
        P("chan", None, "slab", None),
        P("chan", "slab", None),
        P("chan"),
        P("chan"),
    )
    return jax.shard_map(
        local, mesh=mesh, in_specs=placed, out_specs=P(None, "slab", "chan"), check_vma=False
    )
```

```python
import functools
import math

import jax
import jax.numpy as jnp
import numpy as np
from jax import lax
from jax.experimental import pallas as pl
from jax.experimental.pallas import tpu as pltpu
from jax.sharding import PartitionSpec as P

MESH = pl.DeviceIdType.MESH
TERMS = 2
RADIX = 16
LANES = 128
PARTS = 4
NEAR, FAR = 0, 1
HALVES = 4


def fine_tables():
    points = RADIX * LANES
    j = np.arange(RADIX)[:, None, None]
    k = np.arange(LANES)[None, :, None]
    a = np.arange(LANES)[None, None, :]
    angle = 2.0 * np.pi / points * ((a * (RADIX * k + j)) % points)
    cos, sin = np.cos(angle), -np.sin(angle)

    def halves(real, imag):
        table = np.concatenate([real, imag], axis=1).astype(np.float32)
        high = table.astype(jnp.bfloat16)
        low = (table - high.astype(np.float32)).astype(jnp.bfloat16)
        return np.concatenate([high, low], axis=2)

    flip = lambda t: t.transpose(0, 2, 1)
    return halves(cos, sin), halves(flip(cos), -flip(sin))


def swap_table(outer, inner):
    size = outer * inner
    table = np.zeros((size, size), np.float32)
    rows = np.arange(size)
    table[rows, (rows % inner) * outer + rows // inner] = 1.0
    return table.astype(jnp.bfloat16)


def plus(a, b):
    if a is None:
        return b
    return a if b is None else a + b


def minus(a, b):
    if b is None:
        return a
    return -b if a is None else a - b


def times(a, s):
    return None if a is None or s == 0.0 else a * s


def cadd(a, b):
    return plus(a[0], b[0]), plus(a[1], b[1])


def csub(a, b):
    return minus(a[0], b[0]), minus(a[1], b[1])


def turn(a, sign):
    if sign > 0:
        return minus(None, a[1]) if a[1] is not None else None, a[0]
    return a[1], minus(None, a[0]) if a[0] is not None else None


def ctwist(a, step, sign):
    step %= RADIX
    if step == 0:
        return a
    if step == 4:
        return turn(a, sign)
    c, s = math.cos(2 * math.pi * step / RADIX), sign * math.sin(2 * math.pi * step / RADIX)
    if step % 8 == 2:
        return times(minus(a[0], times(a[1], sign)), c), times(plus(times(a[0], sign), a[1]), c)
    return minus(times(a[0], c), times(a[1], s)), plus(times(a[0], s), times(a[1], c))


def four(a, b, c, d, sign):
    t0, t1, t2, t3 = cadd(a, c), csub(a, c), cadd(b, d), turn(csub(b, d), sign)
    return cadd(t0, t2), cadd(t1, t3), csub(t0, t2), csub(t1, t3)


def sixteen(x, sign):
    mid = [four(x[n], x[4 + n], x[8 + n], x[12 + n], sign) for n in range(4)]
    out = [None] * RADIX
    for k in range(4):
        tw = [ctwist(mid[n][k], n * k, sign) for n in range(4)]
        for q, y in enumerate(four(*tw, sign)):
            out[k + 4 * q] = y
    return out


def fine(table, x):
    high = x.astype(jnp.bfloat16)
    low = (x - high.astype(jnp.float32)).astype(jnp.bfloat16)
    t_high, t_low = table[:, :LANES], table[:, LANES:]
    left = jnp.concatenate(
        [jnp.concatenate([t_high, t_high], axis=1), jnp.concatenate([t_low, t_low], axis=1)], axis=0
    )
    out = jnp.dot(left, jnp.concatenate([high, low], axis=0), preferred_element_type=jnp.float32)
    out = out[: 2 * LANES] + out[2 * LANES :]
    n = x.shape[1] // 2
    real = out[:LANES, :n] - out[LANES:, n:]
    imag = out[:LANES, n:] + out[LANES:, :n]
    return real, imag


def put(ref, *index, at, value):
    for part in range(2):
        v = value[part]
        if v is None:
            v = jnp.zeros((8, LANES), jnp.float32)
        ref[(*index, pl.ds(al8(at), 8), pl.ds(part * LANES, LANES))] = v


def get(ref, *index, at):
    return tuple(ref[(*index, pl.ds(al8(at), 8), pl.ds(part * LANES, LANES))] for part in range(2))


def al8(i):
    return pl.multiple_of(i, 8)


def kernel(
    C, S,
    x_hbm, vis_hbm, wt_hbm, freq_ref, rob_ref, fwd_hbm, bwd_hbm, pu_hbm, pv_hbm,
    out_hbm,
    xr, xt, y_s, z_s, w_s, rs, rr, ms, mr, bs, br, ts, tr, x_s, os_, fwd, bwd, pu, pv,
    raw, vt, offs, mine,
    load_sem, x_send, x_recv, x_own, o_send, o_recv, o_own, o_done, f_send, f_recv,
    r_send, r_recv, r_own, m_send, m_recv, m_own, b_send, b_recv, b_own, t_send, t_recv, t_own,
):
    H = rs.shape[0]
    sub = x_hbm.shape[1] // C
    rows, cols = x_hbm.shape[1], x_hbm.shape[2]
    jper = RADIX // H
    kl = LANES // S
    piece = sub // PARTS
    scale = 1.0 / (RADIX * LANES)
    c_me, s_me = lax.axis_index("chan"), lax.axis_index("slab")
    chan_peers = [lax.rem(c_me + d, C) for d in range(1, C)]
    if C == 4:
        chan_peers = [3 - c_me, c_me + 1 - 2 * lax.rem(c_me, 2), lax.rem(c_me + 2, 4)]
    G = S // 2
    low = s_me // G * G
    first_of = (low, G - low)
    slab_peers = (
        [low + lax.rem(s_me + d, G) for d in range(1, G)],
        [G - low + lax.rem(s_me + d, G) for d in range(G)],
    )

    def load(n):
        source, target = (
            (fwd_hbm, fwd),
            (vis_hbm.at[0], raw.at[pl.ds(0, 2)]),
            (wt_hbm, raw.at[pl.ds(2, 1)]),
            (pu_hbm, pu),
            (pv_hbm, pv),
            (bwd_hbm, bwd),
        )[n]
        return pltpu.make_async_copy(source, target, load_sem.at[n])

    def remote(src, dst, send, recv, **where):
        pltpu.make_async_remote_copy(
            src_ref=src, dst_ref=dst, send_sem=send, recv_sem=recv,
            device_id=where, device_id_type=MESH,
        ).start()

    def own(src, dst, sem):
        pltpu.make_async_copy(src, dst, sem).start()

    def landed(ref, sem):
        pltpu.make_async_copy(ref, ref, sem).wait()

    half = sub // HALVES
    halved = lambda p: pl.ds(p * half, half)
    wide = TERMS * half

    mine[...] = jnp.full(mine.shape, freq_ref[0] - 1.0, jnp.float32)
    barrier = pltpu.get_barrier_semaphore()
    for c in chan_peers:
        pl.semaphore_signal(barrier, inc=1, device_id={"chan": c}, device_id_type=MESH)
    for s in slab_peers[NEAR] + slab_peers[FAR]:
        pl.semaphore_signal(barrier, inc=1, device_id={"slab": s}, device_id_type=MESH)
    for p in range(HALVES):
        own(
            x_hbm.at[:, pl.ds(al8(sub * c_me + p * half), half), :],
            xr.at[c_me, :, halved(p), :], x_own.at[p],
        )
    for n in range(6):
        load(n).start()
    pl.semaphore_wait(barrier, C + S - 2)

    own(mine, offs.at[c_me], o_own)
    for c in chan_peers:
        remote(mine, offs.at[c_me], f_send, f_recv, chan=c)

    def send_tiles(p):
        for c in chan_peers:
            remote(
                x_hbm.at[:, pl.ds(al8(sub * c + p * half), half), :],
                xr.at[c_me, :, halved(p), :], x_send, x_recv.at[p], chan=c,
            )

    def prep(which, first, last):
        def body(m, carry):
            block = raw[which, :, pl.ds(pl.multiple_of(m * 256, 256), 256)]
            turned = jnp.dot(pu[...], block, preferred_element_type=jnp.float32)
            flipped = lax.dot_general(
                pv[...], turned.astype(jnp.bfloat16), (((1,), (1,)), ((), ())),
                preferred_element_type=jnp.float32,
            ).astype(jnp.bfloat16)
            for h in range(H):
                for j in range(RADIX):
                    vt[which, h, j, pl.ds(pl.multiple_of(16 * m, 16), 16), :] = flipped[
                        16 * j : 16 * j + 16, LANES * h : LANES * (h + 1)
                    ]
            return carry

        lax.fori_loop(first, last, body, 0)

    def rows_in(p):
        landed(xr.at[pl.ds(0, C - 1), :, halved(p), :], x_recv.at[p])
        landed(xr.at[0, :, halved(p), :], x_own.at[p])
        per = cols // LANES
        for b in range(RADIX):
            tile = xr[b // per, :, halved(p), LANES * (b % per) : LANES * (b % per + 1)]
            xt[b, :, 0:wide] = tile.reshape(wide, LANES).T

        def body(n, carry):
            out = sixteen([(xt[b, pl.ds(al8(8 * n), 8), :], None) for b in range(RADIX)], -1)
            for j in range(RADIX):
                put(y_s, p, j, at=8 * n, value=out[j])
            return carry

        lax.fori_loop(0, LANES // 8, body, 0)

    def rows_out(h, p):
        def body(jl, carry):
            z = fine(fwd[jper * h + jl], y_s[p, jper * h + jl])
            for s in range(S):
                for part in range(2):
                    w_s[s, part, pl.ds(al8(kl * jl), kl), :] = z[part][kl * s : kl * (s + 1), :]
            return carry

        lax.fori_loop(0, jper, body, 0, unroll=4)

        def flip(s, carry):
            for part in range(2):
                rs[h, s, part, :, halved(p), :] = w_s[s, part, :, 0:wide].T.reshape(TERMS, half, LANES)
            return carry

        lax.fori_loop(0, S, flip, 0, unroll=2)

    def to_slabs(source, target, g, n, send, recv, done):
        h, q = n // PARTS, n % PARTS
        span = pl.ds(q * piece, piece)
        for s in slab_peers[g]:
            remote(
                source.at[h, s, :, :, span, :], target.at[h, s_me, :, :, span, :],
                send, recv.at[g, h, q], slab=s,
            )
        if g == NEAR:
            own(
                source.at[h, s_me, :, :, span, :], target.at[h, s_me, :, :, span, :],
                done.at[h, q],
            )

    def from_slabs(target, g, n, recv, done):
        h, q = n // PARTS, n % PARTS
        span = pl.ds(q * piece, piece)
        landed(target.at[h, pl.ds(0, len(slab_peers[g])), :, :, span, :], recv.at[g, h, q])
        if g == NEAR:
            landed(target.at[h, 0, :, :, span, :], done.at[h, q])

    def send_rows(g, n):
        to_slabs(rs, rr, g, n, r_send, r_recv, r_own)

    def mix(g, n):
        h, q = n // PARTS, n % PARTS
        span = pl.ds(q * piece, piece)
        from_slabs(rr, g, n, r_recv, r_own)

        def body(i, carry):
            s = first_of[g] + i
            base = rr[h, s, :, 0, span, :] * scale
            slope = rr[h, s, :, 1, span, :] * scale
            for c in range(C):
                offset = offs[c, 0:1, :]
                ms[h, c, :, s, span, :] = base + offset[None] * slope
            return carry

        lax.fori_loop(0, G, body, 0)
        there = pl.ds(al8(sub * c_me + q * piece), piece)
        group = pl.ds(first_of[g], G)
        for c in chan_peers:
            remote(
                ms.at[h, c, :, group, span, :], mr.at[h, :, group, there, :],
                m_send, m_recv.at[h], chan=c,
            )
        own(ms.at[h, c_me, :, group, span, :], mr.at[h, :, group, there, :], m_own.at[h])

    def column_in(h):
        landed(ms.at[h, pl.ds(0, C - 1)], m_recv.at[h])
        landed(ms.at[h, 0], m_own.at[h])

        def body(n, carry):
            at = 8 * n
            x = []
            for b in range(RADIX):
                s, row = LANES * b // rows, LANES * b % rows
                x.append(tuple(mr[h, part, s, pl.ds(al8(row + at), 8), :] for part in range(2)))
            out = sixteen(x, -1)
            for j in range(RADIX):
                put(y_s, h, j, at=at, value=out[j])
            return carry

        lax.fori_loop(0, LANES // 8, body, 0)

    def column_mid(h, first, last):
        def body(j, carry):
            zr, zi = fine(fwd[j], y_s[h, j])
            weight = vt[2, h, j].astype(jnp.float32)
            real = vt[0, h, j].astype(jnp.float32) - weight * zr
            imag = vt[1, h, j].astype(jnp.float32) - weight * zi
            robust = 1.0 / (1.0 + rob_ref[0] * (real * real + imag * imag))
            zr, zi = fine(bwd[j], jnp.concatenate([robust * real, robust * imag], axis=1))
            z_s[h, j, :, 0:LANES] = zr
            z_s[h, j, :, LANES : 2 * LANES] = zi
            return carry

        lax.fori_loop(first, last, body, 0, unroll=4)

    def column_out(h):
        def body(n, carry):
            out = sixteen([get(z_s, h, j, at=8 * n) for j in range(RADIX)], 1)
            for b in range(RADIX):
                s, row = LANES * b // rows, LANES * b % rows
                for part in range(2):
                    bs[h, part, s, pl.ds(al8(row + 8 * n), 8), :] = out[b][part]
            return carry

        lax.fori_loop(0, LANES // 8, body, 0)

    def send_back(g, n):
        h, q = n // PARTS, n % PARTS
        span = pl.ds(q * piece, piece)
        group = pl.ds(first_of[g], G)
        here = lambda c: pl.ds(al8(sub * c + q * piece), piece)
        for c in chan_peers:
            remote(
                bs.at[h, :, group, here(c), :], br.at[h, c_me, :, group, span, :],
                b_send, b_recv.at[g, h, q], chan=c,
            )
        own(
            bs.at[h, :, group, here(c_me), :], br.at[h, c_me, :, group, span, :],
            b_own.at[g, h, q],
        )

    arrived = set()

    def returned(g, n):
        if (g, n) not in arrived:
            arrived.add((g, n))
            from_slabs(tr, g, n, t_recv, t_own)

    def gather(g, n):
        h, q = n // PARTS, n % PARTS
        span = pl.ds(q * piece, piece)
        group = pl.ds(first_of[g], G)
        landed(br.at[h, pl.ds(0, C - 1), :, group, span, :], b_recv.at[g, h, q])
        landed(br.at[h, 0, :, group, span, :], b_own.at[g, h, q])

        def body(i, carry):
            s = first_of[g] + i
            base, slope = None, None
            for c in range(C):
                offset = (offs[c, 0:1, :])[None]
                value = br[h, c, :, s, span, :]
                base = value if base is None else base + value
                slope = offset * value if slope is None else slope + offset * value
            ts[h, s, :, 0, span, :] = base
            ts[h, s, :, 1, span, :] = slope
            return carry

        lax.fori_loop(0, G, body, 0)
        to_slabs(ts, tr, g, n, t_send, t_recv, t_own)

    def back_in(h, p):
        returned(FAR, h * PARTS + p)
        returned(NEAR, h * PARTS + p)

        def flip(s, carry):
            for part in range(2):
                tile = tr[h, s, part, :, halved(p), :].reshape(wide, LANES).T
                for jl in range(jper):
                    x_s[jl, pl.ds(al8(kl * s), kl), part * LANES : part * LANES + wide] = tile[
                        kl * jl : kl * (jl + 1), :
                    ]
            return carry

        lax.fori_loop(0, S, flip, 0, unroll=2)

        def body(jl, carry):
            zr, zi = fine(bwd[jper * h + jl], x_s[jl])
            y_s[p, jper * h + jl, :, 0:LANES] = zr
            y_s[p, jper * h + jl, :, LANES : 2 * LANES] = zi
            return carry

        lax.fori_loop(0, jper, body, 0, unroll=4)

    def back_out(p):
        def body(n, carry):
            out = sixteen([get(y_s, p, j, at=8 * n) for j in range(RADIX)], 1)
            for b in range(RADIX):
                xt[b, pl.ds(al8(8 * n), 8), :] = out[b][0]
            return carry

        lax.fori_loop(0, LANES // 8, body, 0)
        per = cols // LANES
        for b in range(RADIX):
            os_[b // per, :, halved(p), LANES * (b % per) : LANES * (b % per + 1)] = (
                xt[b, :, 0:wide].T.reshape(TERMS, half, LANES)
            )
        there = pl.ds(al8(sub * c_me + p * half), half)
        for c in chan_peers:
            remote(os_.at[c, :, halved(p), :], out_hbm.at[:, there, :], o_send, o_recv, chan=c)
        own(os_.at[c_me, :, halved(p), :], out_hbm.at[:, there, :], o_done)

    for p in range(HALVES):
        send_tiles(p)
    for n in range(1, 5):
        load(n).wait()
    prep(0, 0, 8)
    load(0).wait()
    load(5).wait()
    landed(offs.at[0], o_own)
    rows_in(0)
    rows_out(0, 0)
    send_rows(NEAR, 0)
    send_rows(FAR, 0)
    rows_in(1)
    rows_out(0, 1)
    send_rows(NEAR, 1)
    send_rows(FAR, 1)
    landed(offs.at[pl.ds(0, C - 1)], f_recv)
    mix(NEAR, 0)
    rows_in(2)
    rows_out(0, 2)
    send_rows(NEAR, 2)
    mix(NEAR, 1)
    rows_in(3)
    rows_out(0, 3)
    send_rows(NEAR, 3)
    mix(FAR, 0)
    send_rows(FAR, 2)
    mix(NEAR, 2)
    rows_out(1, 0)
    mix(NEAR, 3)
    prep(1, 0, 4)
    mix(FAR, 1)
    send_rows(FAR, 3)
    rows_out(1, 1)
    prep(1, 4, 8)
    rows_out(1, 2)
    mix(FAR, 2)
    send_rows(NEAR, 4)
    send_rows(FAR, 4)
    rows_out(1, 3)
    prep(2, 0, 4)
    mix(FAR, 3)
    send_rows(NEAR, 5)
    send_rows(FAR, 5)
    mix(NEAR, 4)
    prep(2, 4, 8)
    mix(NEAR, 5)
    column_in(0)
    mix(FAR, 4)
    send_rows(NEAR, 6)
    send_rows(FAR, 6)
    column_mid(0, 0, 8)
    mix(FAR, 5)
    send_rows(NEAR, 7)
    send_rows(FAR, 7)
    column_mid(0, 8, 16)
    column_out(0)
    send_back(FAR, 0)
    mix(NEAR, 6)
    send_back(FAR, 1)
    mix(FAR, 6)
    send_back(FAR, 2)
    mix(NEAR, 7)
    gather(FAR, 0)
    mix(FAR, 7)
    send_back(FAR, 3)
    gather(FAR, 1)
    send_back(NEAR, 0)
    gather(FAR, 2)
    send_back(NEAR, 1)
    column_in(1)
    column_mid(1, 0, 8)
    gather(FAR, 3)
    column_mid(1, 8, 16)
    column_out(1)
    send_back(FAR, 4)
    gather(NEAR, 0)
    gather(NEAR, 1)
    send_back(FAR, 5)
    send_back(FAR, 6)
    send_back(FAR, 7)
    gather(FAR, 4)
    send_back(NEAR, 4)
    gather(FAR, 5)
    send_back(NEAR, 5)
    back_in(0, 0)
    send_back(NEAR, 2)
    gather(FAR, 6)
    send_back(NEAR, 6)
    back_in(0, 1)
    gather(FAR, 7)
    send_back(NEAR, 3)
    send_back(NEAR, 7)
    gather(NEAR, 4)
    gather(NEAR, 5)
    back_in(1, 0)
    back_out(0)
    gather(NEAR, 2)
    back_in(1, 1)
    back_out(1)
    gather(NEAR, 6)
    back_in(0, 2)
    gather(NEAR, 3)
    back_in(1, 2)
    back_out(2)
    gather(NEAR, 7)
    back_in(0, 3)
    back_in(1, 3)
    back_out(3)

    landed(xr.at[pl.ds(0, C - 1)], x_send)
    landed(offs.at[pl.ds(0, C - 1)], f_send)
    landed(rs.at[:, pl.ds(0, S - 1)], r_send)
    landed(ms.at[:, pl.ds(0, C - 1)], m_send)
    landed(br.at[:, pl.ds(0, C - 1)], b_send)
    landed(ts.at[:, pl.ds(0, S - 1)], t_send)
    landed(os_.at[pl.ds(0, C - 1)], o_send)
    landed(os_.at[pl.ds(0, C - 1)], o_recv)
    landed(os_.at[0], o_done)


def tiled(taylor_models, gridded_vis, uv_weight, freq_ratio, robust_scale):
    C, S = lax.axis_size("chan"), lax.axis_size("slab")
    terms, rows, cols = taylor_models.shape
    sub = rows // C
    U = gridded_vis.shape[2]
    H = U // LANES
    fwd, bwd = fine_tables()
    pu, pv = swap_table(RADIX, U // RADIX), swap_table(RADIX, 16)
    f32, bf16 = jnp.float32, jnp.bfloat16
    stage = (RADIX, LANES, 2 * LANES)
    slabbed = (H, S, 2, terms, sub, LANES)
    chanbed = (H, C, 2, S, sub, LANES)
    natural = (H, 2, S, rows, LANES)
    V = lambda shape, dtype=f32: pltpu.VMEM(shape, dtype)
    D = pltpu.SemaphoreType.DMA
    anywhere = pl.BlockSpec(memory_space=pl.ANY)
    image = pl.pallas_call(
        functools.partial(kernel, C, S),
        out_shape=jax.ShapeDtypeStruct(taylor_models.shape, f32),
        in_specs=[
            anywhere, anywhere, anywhere,
            pl.BlockSpec(memory_space=pltpu.SMEM), pl.BlockSpec(memory_space=pltpu.SMEM),
            anywhere, anywhere, anywhere, anywhere,
        ],
        out_specs=anywhere,
        scratch_shapes=[
            V((C, terms, sub, cols)), V((RADIX, LANES, LANES)), V((HALVES, *stage)), V((H, *stage)),
            V((S, 2, LANES, LANES)), V(slabbed), V(slabbed), V(chanbed), V(natural),
            V(natural), V(chanbed), V(slabbed), V(slabbed), V((RADIX // H, LANES, 2 * LANES)),
            V((C, terms, sub, cols)), V(fwd.shape, bf16), V(bwd.shape, bf16),
            V(pu.shape, bf16), V(pv.shape, bf16),
            V((3, U, RADIX * LANES), bf16), V((3, H, RADIX, LANES, LANES), bf16),
            V((C, 8, LANES)), V((8, LANES)),
            D((6,)), D(()), D((HALVES,)), D((HALVES,)), D(()), D(()), D(()), D(()), D(()), D(()),
            D(()), D((2, H, PARTS)), D((H, PARTS)),
            D(()), D((H,)), D((H,)),
            D(()), D((2, H, PARTS)), D((2, H, PARTS)),
            D(()), D((2, H, PARTS)), D((H, PARTS)),
        ],
        compiler_params=pltpu.CompilerParams(
            collective_id=0, has_side_effects=True, vmem_limit_bytes=63 * 1024 * 1024
        ),
    )(taylor_models, gridded_vis, uv_weight, freq_ratio, robust_scale, fwd, bwd, pu, pv)
    return image * (1.0 / (RADIX * LANES))


HIGHEST = lax.Precision.HIGH


def dft_table(points, direction):
    steps_all = jnp.arange(points, dtype=jnp.int32)
    product = steps_all[:, None] * steps_all[None, :] % points
    angles = product.astype(jnp.float32) * (2.0 * math.pi / points)
    return (jnp.cos(angles), direction * jnp.sin(angles))


def twiddle_table(outer_points, inner_points, direction):
    outer_steps = jnp.arange(outer_points, dtype=jnp.int32)
    inner_steps = jnp.arange(inner_points, dtype=jnp.int32)
    overall = outer_points * inner_points
    product = outer_steps[:, None] * inner_steps[None, :] % overall
    angles = product.astype(jnp.float32) * (2.0 * math.pi / overall)
    return (jnp.cos(angles), direction * jnp.sin(angles))


def complex_product(formula, left_real, left_imag, table_real, table_imag):
    out_real = jnp.einsum(formula, left_real, table_real, precision=HIGHEST) - jnp.einsum(
        formula, left_imag, table_imag, precision=HIGHEST
    )
    out_imag = jnp.einsum(formula, left_real, table_imag, precision=HIGHEST) + jnp.einsum(
        formula, left_imag, table_real, precision=HIGHEST
    )
    return (out_real, out_imag)


def rotate(left_real, left_imag, table_real, table_imag):
    return (
        left_real * table_real - left_imag * table_imag,
        left_real * table_imag + left_imag * table_real,
    )


def general(taylor_models, gridded_vis, uv_weight, freq_ratio, robust_scale):
    inner_count = 128
    PIX = taylor_models.shape[2] * lax.axis_size("chan")
    outer_count = PIX // inner_count
    chans = lax.axis_size("chan")
    slabs = lax.axis_size("slab")
    rows = taylor_models.shape[1]
    cols = taylor_models.shape[2]
    sub = rows // chans
    col_count = PIX // slabs
    outer_cos, outer_sin = dft_table(outer_count, -1.0)
    inner_cos, inner_sin = dft_table(inner_count, -1.0)
    twist_cos, twist_sin = twiddle_table(outer_count, inner_count, -1.0)
    offsets = lax.all_gather(freq_ratio, "chan", axis=0, tiled=True) - 1.0

    pieces = taylor_models.reshape(TERMS, chans, sub, cols).transpose(1, 0, 2, 3)
    pieces = lax.all_to_all(pieces, "chan", split_axis=0, concat_axis=0, tiled=True)
    layered = pieces.transpose(1, 2, 0, 3).reshape(TERMS * sub, outer_count, inner_count)
    part_real = jnp.einsum("yba,jb->yja", layered, outer_cos, precision=HIGHEST)
    part_imag = jnp.einsum("yba,jb->yja", layered, outer_sin, precision=HIGHEST)
    turned_real, turned_imag = rotate(part_real, part_imag, twist_cos, twist_sin)
    spec_real, spec_imag = complex_product(
        "yja,ka->kjy", turned_real, turned_imag, inner_cos, inner_sin
    )
    outgoing = jnp.stack(
        [
            spec_real.reshape(slabs, col_count, TERMS * sub),
            spec_imag.reshape(slabs, col_count, TERMS * sub),
        ],
        axis=1,
    )
    arrived = lax.all_to_all(outgoing, "slab", split_axis=0, concat_axis=0, tiled=True)
    arrived = arrived.reshape(slabs, 2, col_count, TERMS, sub)
    arrived = arrived.transpose(3, 1, 2, 0, 4).reshape(TERMS, 2, col_count, slabs * sub)
    mixed = arrived[0][None] + offsets[:, None, None, None] * arrived[1][None]
    mixed = lax.all_to_all(mixed, "chan", split_axis=0, concat_axis=0, tiled=True)
    columns = mixed.reshape(chans, 2, col_count, slabs, sub).transpose(1, 2, 3, 0, 4)
    layered_cols = columns.reshape(2, col_count, outer_count, inner_count)
    part_real, part_imag = complex_product(
        "uba,jb->uja", layered_cols[0], layered_cols[1], outer_cos, outer_sin
    )
    turned_real, turned_imag = rotate(part_real, part_imag, twist_cos, twist_sin)
    freq_real, freq_imag = complex_product(
        "uja,ka->ujk", turned_real, turned_imag, inner_cos, inner_sin
    )
    freq_real = freq_real / PIX
    freq_imag = freq_imag / PIX
    weight = (
        uv_weight[0]
        .astype(jnp.float32)
        .reshape(col_count, inner_count, outer_count)
        .transpose(0, 2, 1)
    )
    visible = (
        gridded_vis[0]
        .astype(jnp.float32)
        .reshape(2, col_count, inner_count, outer_count)
        .transpose(0, 1, 3, 2)
    )
    delta_real = visible[0] - weight * freq_real
    delta_imag = visible[1] - weight * freq_imag
    robust = 1.0 / (1.0 + robust_scale[0] * (delta_real * delta_real + delta_imag * delta_imag))
    weighted_real = robust * delta_real
    weighted_imag = robust * delta_imag
    back_real, back_imag = complex_product(
        "ujk,ak->uja", weighted_real, weighted_imag, inner_cos, -inner_sin
    )
    back_real, back_imag = rotate(back_real, back_imag, twist_cos, -twist_sin)
    back_real, back_imag = complex_product(
        "uja,bj->uba", back_real, back_imag, outer_cos, -outer_sin
    )
    back = jnp.stack([back_real, back_imag]).reshape(2, col_count, slabs, chans, sub)
    back = back.transpose(3, 0, 1, 2, 4).reshape(chans, 2, col_count, slabs * sub)
    back = lax.all_to_all(back, "chan", split_axis=0, concat_axis=0, tiled=True)
    total = jnp.stack(
        [jnp.sum(back * offsets[:, None, None, None] ** t, axis=0) for t in range(TERMS)]
    )
    total = total.reshape(TERMS, 2, col_count, slabs, sub).transpose(3, 1, 2, 0, 4)
    total = total.reshape(slabs, 2, col_count, TERMS * sub)
    total = lax.all_to_all(total, "slab", split_axis=0, concat_axis=0, tiled=True)
    layered_rows = total.transpose(1, 0, 2, 3).reshape(2, inner_count, outer_count, TERMS * sub)
    last_real, last_imag = complex_product(
        "kjy,ak->ajy", layered_rows[0], layered_rows[1], inner_cos, -inner_sin
    )
    last_real, last_imag = rotate(
        last_real, last_imag, twist_cos.T[:, :, None], -twist_sin.T[:, :, None]
    )
    image_out = jnp.einsum("ajy,bj->yba", last_real, outer_cos, precision=HIGHEST) + jnp.einsum(
        "ajy,bj->yba", last_imag, outer_sin, precision=HIGHEST
    )
    image_out = image_out.reshape(TERMS, sub, chans, cols).transpose(2, 0, 1, 3) / PIX
    tiles = lax.all_to_all(image_out, "chan", split_axis=0, concat_axis=0, tiled=True)
    return tiles.transpose(1, 0, 2, 3).reshape(TERMS, rows, cols)


def local(taylor_models, gridded_vis, uv_weight, freq_ratio, robust_scale):
    C, S = lax.axis_size("chan"), lax.axis_size("slab")
    terms, rows, cols = taylor_models.shape
    pix, sub, U = cols * C, rows // C, gridded_vis.shape[2]
    fits = (
        terms == TERMS
        and pix == RADIX * LANES
        and rows * S == pix
        and rows % LANES == 0
        and cols % LANES == 0
        and terms * sub == LANES
        and sub % (8 * PARTS) == 0
        and LANES % (8 * S) == 0
        and S % 2 == 0
        and PARTS == HALVES
        and U == 2 * LANES
    )
    form = tiled if fits else general
    return form(taylor_models, gridded_vis, uv_weight, freq_ratio, robust_scale)


def solution(mesh):
    placed = (
        P(None, "slab", "chan"),
        P("chan", None, "slab", None),
        P("chan", "slab", None),
        P("chan"),
        P("chan"),
    )
    return jax.shard_map(
        local, mesh=mesh, in_specs=placed, out_specs=P(None, "slab", "chan"), check_vma=False
    )
```
